8 devices in a mesh: dp: 2 (over z, y), ep: 4 (over x, core).
Axes of the slice: x: 2, y: 2, z: 1, core: 2. Of those that a mesh axis runs over, the one named last changes fastest.
Arguments:
- grad_y: bfloat16 [512, 1024], P(('dp', 'ep')), parts along dimension 0
- gate_vals: float32 [512, 8], P(('dp', 'ep')), parts along dimension 0
- topk_idx: int32 [512, 8], P(('dp', 'ep')), parts along dimension 0
- slot_ids: int32 [512, 8], P(('dp', 'ep')), parts along dimension 0
- pair_counts: int32 [8, 32], P(('dp', 'ep')), parts along dimension 0
- y_routed: bfloat16 [512, 8, 1024], P(('dp', 'ep')), parts along dimension 0
- x_disp: bfloat16 [64, 128, 1024], P(('dp', 'ep')), parts along dimension 0
- h_gate: bfloat16 [64, 128, 512], P(('dp', 'ep')), parts along dimension 0
- h_up: bfloat16 [64, 128, 512], P(('dp', 'ep')), parts along dimension 0
- w_gate: bfloat16 [32, 1024, 512], P('ep')
- w_up: bfloat16 [32, 1024, 512], P('ep')
- w_down: bfloat16 [32, 512, 1024], P('ep')
Outputs:
- output 1: bfloat16 [512, 1024], P(('dp', 'ep')), parts along dimension 0
- output 2: float32 [512, 8], P(('dp', 'ep')), parts along dimension 0
- output 3: float32 [64, 1024, 512], P(('dp', 'ep')), parts along dimension 0
- output 4: float32 [64, 1024, 512], P(('dp', 'ep')), parts along dimension 0
- output 5: float32 [64, 512, 1024], P(('dp', 'ep')), parts along dimension 0
There are 2 independent parts. The reference program is written for one: setup_inputs(seed, part) draws one part's arguments, and reference() takes and returns one part's arrays. A program takes and returns all parts, laid end to end along the dimension named above; an argument that names none is the same for every part.
All inputs are finite; a program needn't handle non-finite values.
Results may differ from the reference program's by a relative error of at most 0.0149174.
Values are sent between devices in bfloat16 or wider.
A program may use at most 1 GiB of HBM per device.

```python
import jax
import jax.numpy as jnp
from jax import lax

GROUP_DEV = 4
TOKENS_DEV = 64
EXPERTS = 32
TOP_K = 8
MODEL_DIM = 1024
FFN_DIM = 512
CAPACITY = 32
N_TOKENS = GROUP_DEV * TOKENS_DEV
EXPERT_ROWS = GROUP_DEV * CAPACITY


def setup_inputs(seed: int = 0, part: int = 0) -> dict:
    base_key = jax.random.fold_in(jax.random.key(seed), part)
    key_list = jax.random.split(base_key, 8)
    weight_keys = jax.random.split(jax.random.key(seed + 1), 3)
    key_noise, key_bias, key_hot = jax.random.split(key_list[0], 3)
    expert_iota = jnp.arange(EXPERTS, dtype=jnp.int32)
    token_iota = jnp.arange(TOKENS_DEV, dtype=jnp.int32)
    noise_int = jax.random.randint(key_noise, (GROUP_DEV, TOKENS_DEV, EXPERTS), 0, 4 * EXPERTS)
    bias_base = jax.random.randint(key_bias, (EXPERTS,), 0, 2 * EXPERTS)
    bias_int = (bias_base * bias_base) // (4 * EXPERTS)
    hot_expert = jax.random.randint(key_hot, (GROUP_DEV,), 0, EXPERTS)
    hot_bonus = jnp.where((token_iota[None, :, None] < CAPACITY) & (expert_iota[None, None, :] == hot_expert[:, None, None]), 8 * EXPERTS, 0)
    scores = (noise_int + bias_int[None, None, :] + hot_bonus) * EXPERTS + expert_iota[None, None, :]
    expert_ids = lax.top_k(scores, TOP_K)[1].astype(jnp.int32)

    def rank_one(ids_dev):
        flat_ids = ids_dev.reshape(-1)
        onehot = (flat_ids[:, None] == expert_iota[None, :]).astype(jnp.int32)
        before = jnp.cumsum(onehot, axis=0) - onehot
        rank_pos = jnp.sum(before * onehot, axis=1)
        return rank_pos.reshape(TOKENS_DEV, TOP_K), jnp.sum(onehot, axis=0)

    rank_pos, n_total = lax.map(rank_one, expert_ids)
    slot_dev = jnp.where(rank_pos < CAPACITY, rank_pos, -1).astype(jnp.int32)
    pair_counts = jnp.minimum(n_total, CAPACITY).astype(jnp.int32)
    is_kept = slot_dev >= 0
    slot_safe = jnp.where(is_kept, slot_dev, CAPACITY)
    slot_clip = jnp.where(is_kept, slot_dev, 0)
    src_dev = jnp.broadcast_to(jnp.arange(GROUP_DEV, dtype=jnp.int32)[:, None, None], expert_ids.shape)

    w_gate = (jax.random.normal(weight_keys[0], (EXPERTS, MODEL_DIM, FFN_DIM), jnp.float32) * MODEL_DIM ** -0.5).astype(jnp.bfloat16)
    w_up = (jax.random.normal(weight_keys[1], (EXPERTS, MODEL_DIM, FFN_DIM), jnp.float32) * MODEL_DIM ** -0.5).astype(jnp.bfloat16)
    w_down = (jax.random.normal(weight_keys[2], (EXPERTS, FFN_DIM, MODEL_DIM), jnp.float32) * FFN_DIM ** -0.5).astype(jnp.bfloat16)
    x_tok = jax.random.normal(key_list[1], (GROUP_DEV, TOKENS_DEV, MODEL_DIM), jnp.float32).astype(jnp.bfloat16)
    stale_rows = jax.random.normal(key_list[2], (EXPERTS, GROUP_DEV, CAPACITY, MODEL_DIM), jnp.float32).astype(jnp.bfloat16)
    x_vals = jnp.broadcast_to(x_tok[:, :, None, :], (GROUP_DEV, TOKENS_DEV, TOP_K, MODEL_DIM))
    x_disp = stale_rows.at[expert_ids, src_dev, slot_safe].set(x_vals, mode="drop").reshape(EXPERTS, EXPERT_ROWS, MODEL_DIM)

    def forward_one(operands):
        x_rows, w_gate_e, w_up_e, w_down_e = operands
        h_g = jnp.dot(x_rows, w_gate_e, preferred_element_type=jnp.float32).astype(jnp.bfloat16)
        h_u = jnp.dot(x_rows, w_up_e, preferred_element_type=jnp.float32).astype(jnp.bfloat16)
        gate_f = h_g.astype(jnp.float32)
        hidden_act = (gate_f * jax.nn.sigmoid(gate_f) * h_u.astype(jnp.float32)).astype(jnp.bfloat16)
        y_rows = jnp.dot(hidden_act, w_down_e, preferred_element_type=jnp.float32).astype(jnp.bfloat16)
        return h_g, h_u, y_rows

    h_gate, h_up, y_exp = lax.map(forward_one, (x_disp, w_gate, w_up, w_down))
    y_pick = y_exp.reshape(EXPERTS, GROUP_DEV, CAPACITY, MODEL_DIM)[expert_ids, src_dev, slot_clip]
    y_routed = jnp.where(is_kept[..., None], y_pick, jnp.zeros((), jnp.bfloat16)).reshape(N_TOKENS, TOP_K, MODEL_DIM)
    grad_y = jax.random.normal(key_list[3], (N_TOKENS, MODEL_DIM), jnp.float32).astype(jnp.bfloat16)
    gate_vals = jax.random.uniform(key_list[4], (N_TOKENS, TOP_K), jnp.float32, 0.25, 1.0)
    return {"grad_y": grad_y, "gate_vals": gate_vals, "topk_idx": expert_ids.reshape(N_TOKENS, TOP_K), "slot_ids": slot_dev.reshape(N_TOKENS, TOP_K), "pair_counts": pair_counts, "y_routed": y_routed, "x_disp": x_disp, "h_gate": h_gate, "h_up": h_up, "w_gate": w_gate, "w_up": w_up, "w_down": w_down}


def reference(grad_y, gate_vals, topk_idx, slot_ids, pair_counts, y_routed, x_disp, h_gate, h_up, w_gate, w_up, w_down):
    grad_gate = jnp.einsum("td,tkd->tk", grad_y.astype(jnp.float32), y_routed.astype(jnp.float32))
    is_kept = slot_ids >= 0
    src_dev = jnp.broadcast_to((jnp.arange(N_TOKENS, dtype=jnp.int32) // TOKENS_DEV)[:, None], topk_idx.shape)
    slot_safe = jnp.where(is_kept, slot_ids, CAPACITY)
    slot_clip = jnp.where(is_kept, slot_ids, 0)
    gated_rows = (gate_vals[:, :, None] * grad_y.astype(jnp.float32)[:, None, :]).astype(jnp.bfloat16)
    disp_rows = jnp.zeros((EXPERTS, GROUP_DEV, CAPACITY, MODEL_DIM), jnp.bfloat16).at[topk_idx, src_dev, slot_safe].set(gated_rows, mode="drop")
    keep_row = jnp.arange(CAPACITY)[None, None, :] < jnp.transpose(pair_counts)[:, :, None]
    disp_rows = jnp.where(keep_row[..., None], disp_rows, jnp.zeros((), jnp.bfloat16)).reshape(EXPERTS, EXPERT_ROWS, MODEL_DIM)

    def expert_one(operands):
        grad_rows, x_rows, hg_rows, hu_rows, w_gate_e, w_up_e, w_down_e = operands
        grad_hidden = jnp.dot(grad_rows, w_down_e.T, preferred_element_type=jnp.float32).astype(jnp.bfloat16)
        gate_f = hg_rows.astype(jnp.float32)
        up_f = hu_rows.astype(jnp.float32)
        gate_sig = jax.nn.sigmoid(gate_f)
        gate_act = gate_f * gate_sig
        hidden_act = (gate_act * up_f).astype(jnp.bfloat16)
        grad_h = grad_hidden.astype(jnp.float32)
        grad_hgate = (grad_h * up_f * gate_sig * (1.0 + gate_f * (1.0 - gate_sig))).astype(jnp.bfloat16)
        grad_hup = (grad_h * gate_act).astype(jnp.bfloat16)
        grad_wdown = jnp.dot(hidden_act.T, grad_rows, preferred_element_type=jnp.float32)
        grad_wgate = jnp.dot(x_rows.T, grad_hgate, preferred_element_type=jnp.float32)
        grad_wup = jnp.dot(x_rows.T, grad_hup, preferred_element_type=jnp.float32)
        grad_disp = (jnp.dot(grad_hgate, w_gate_e.T, preferred_element_type=jnp.float32) + jnp.dot(grad_hup, w_up_e.T, preferred_element_type=jnp.float32)).astype(jnp.bfloat16)
        return grad_disp, grad_wgate, grad_wup, grad_wdown

    grad_disp, grad_w_gate, grad_w_up, grad_w_down = lax.map(expert_one, (disp_rows, x_disp, h_gate, h_up, w_gate, w_up, w_down))
    back_rows = grad_disp.reshape(EXPERTS, GROUP_DEV, CAPACITY, MODEL_DIM)[topk_idx, src_dev, slot_clip]
    grad_x = jnp.sum(jnp.where(is_kept[..., None], back_rows.astype(jnp.float32), 0.0), axis=1).astype(jnp.bfloat16)
    return grad_x, grad_gate, grad_w_gate, grad_w_up, grad_w_down
```

```python
import jax
import jax.numpy as jnp
from jax import lax
from jax.experimental import pallas as pl
from jax.experimental.pallas import tpu as pltpu
from jax.sharding import PartitionSpec as P

MESH_ID = pl.DeviceIdType.MESH
F32 = jnp.float32
BF16 = jnp.bfloat16
NT = (((1,), (1,)), ((), ()))
TN = (((0,), (0,)), ((), ()))


def token_kernel(gy, gv, tk, sl, pc, yr, hg, hu, wg, wu, wd,
                 part, dd, aa, dh, gg,
                 gy_all, gv_all, tk_all, sl_all, pc_all, yr_v, hg_v, hu_v, wg_v, wu_v, wd_v,
                 c1_v, s_v, p_all, r_all,
                 own_sem, bulk_sem, wd_sem, wg_sem, wu_sem,
                 gs_sem, gr_sem, ss_sem, sr_sem):
    n_loc = wd.shape[0]
    cap = dd.shape[2]
    tok, dim = gy.shape
    ffn = wd.shape[1]
    half = tok // 2
    me = lax.axis_index("ep")
    partner = me + 1 - 2 * lax.rem(me, 2)
    far = lax.rem(me + 2, 4)
    far_partner = lax.rem(partner + 2, 4)
    peers = (partner, far, far_partner)

    own = [pltpu.make_async_copy(gy, gy_all.at[me], own_sem.at[0]),
           pltpu.make_async_copy(gv, gv_all.at[me], own_sem.at[1]),
           pltpu.make_async_copy(tk, tk_all.at[me], own_sem.at[2]),
           pltpu.make_async_copy(sl, sl_all.at[me], own_sem.at[3]),
           pltpu.make_async_copy(pc, pc_all.at[me], own_sem.at[4])]
    for c in own:
        c.start()
    barrier = pltpu.get_barrier_semaphore()
    for d in peers:
        pl.semaphore_signal(barrier, inc=1, device_id={"ep": d}, device_id_type=MESH_ID)
    bulk = [pltpu.make_async_copy(hg, hg_v, bulk_sem.at[0]),
            pltpu.make_async_copy(hu, hu_v, bulk_sem.at[1]),
            pltpu.make_async_copy(yr, yr_v, bulk_sem.at[2])]
    for c in bulk:
        c.start(priority=1)
    for e in range(n_loc):
        pltpu.make_async_copy(wd.at[e], wd_v.at[e], wd_sem.at[e]).start(priority=1)
    for e in range(n_loc):
        pltpu.make_async_copy(wg.at[e], wg_v.at[e], wg_sem.at[e]).start(priority=1)
        pltpu.make_async_copy(wu.at[e], wu_v.at[e], wu_sem.at[e]).start(priority=1)
    for c in own:
        c.wait()
    pl.semaphore_wait(barrier, 3)

    def remote(src, dst, ssem, rsem, dev):
        return pltpu.make_async_remote_copy(src_ref=src, dst_ref=dst, send_sem=ssem, recv_sem=rsem, device_id={"ep": dev}, device_id_type=MESH_ID)

    small = []
    for i, d in enumerate(peers):
        for k, ref in enumerate((gv_all, tk_all, sl_all, pc_all)):
            c = remote(ref.at[me], ref.at[me], ss_sem.at[i, k], sr_sem.at[i, k], d)
            c.start()
            small.append(c)
    to_far = []
    for h in range(2):
        rows = pl.ds(h * half, half)
        c = remote(gy_all.at[me, rows], gy_all.at[me, rows], gs_sem.at[1 + h], gr_sem.at[1 + h], far)
        c.start()
        to_far.append(c)
    to_partner = remote(gy_all.at[me], gy_all.at[me], gs_sem.at[0], gr_sem.at[0], partner)
    to_partner.start()

    def build(s):
        ids = tk_all[s]
        slots = sl_all[s]
        gates = gv_all[s]
        counts = pc_all[s]
        lane = lax.broadcasted_iota(jnp.int32, counts.shape, 1)
        row_c = lax.broadcasted_iota(jnp.int32, (cap, tok), 0).astype(F32)
        hots, cols = [], []
        for e in range(n_loc):
            g = me * n_loc + e
            cnt = jnp.sum(jnp.where(lane == g, counts.astype(F32), 0.0), axis=1, keepdims=True)
            slots_f = slots.astype(F32)
            ok = (ids == g) & (slots >= 0) & (slots_f < cnt)
            slot_row = jnp.max(jnp.where(ok, slots_f, -1.0), axis=0, keepdims=True)
            gate_row = jnp.sum(jnp.where(ok, gates, 0.0), axis=0, keepdims=True)
            hit = row_c == slot_row
            cols.append(jnp.sum(jnp.where(hit, gate_row, 0.0), axis=1, keepdims=True))
            hots.append(jnp.where(hit, 1.0, 0.0).astype(BF16))
        hot = jnp.concatenate(hots, axis=0)
        p_all[s] = hot
        for n in range(0, dim, 256):
            picked = jnp.dot(hot, gy_all[s, :, n:n + 256], preferred_element_type=F32)
            for e in range(n_loc):
                dd[e, s, :, n:n + 256] = (picked[e * cap:(e + 1) * cap] * cols[e]).astype(BF16)

    build(me)

    bulk[0].wait()
    bulk[1].wait()

    def pre(e, carry):
        h1 = hg_v[e].astype(F32)
        h3 = hu_v[e].astype(F32)
        sig = jax.nn.sigmoid(h1)
        act = h1 * sig
        aa[e] = (act * h3).astype(BF16)
        c1_v[e] = h3 * sig * (1.0 + h1 * (1.0 - sig))
        s_v[e] = act
        return carry

    lax.fori_loop(0, n_loc, pre, 0)

    bulk[2].wait()
    top_k = yr.shape[1]
    dots = lax.dot_general(yr_v[...].reshape(tok * top_k, dim), gy_all[me], NT, preferred_element_type=F32).reshape(tok, top_k, tok)
    same = lax.broadcasted_iota(jnp.int32, dots.shape, 0) == lax.broadcasted_iota(jnp.int32, dots.shape, 2)
    gg[...] = jnp.sum(jnp.where(same, dots, 0.0), axis=0)

    for k in range(4):
        small[k].wait_recv()
    to_partner.wait_recv()
    build(partner)

    relay = []
    for h in range(2):
        rows = pl.ds(h * half, half)
        to_far[h].wait_recv()
        c = remote(gy_all.at[far, rows], gy_all.at[far, rows], gs_sem.at[3 + h], gr_sem.at[3 + h], partner)
        c.start()
        relay.append(c)
    for k in range(4):
        small[4 + k].wait_recv()
    build(far)
    for k in range(4):
        small[8 + k].wait_recv()
    for h in range(2):
        relay[h].wait_recv()
    build(far_partner)

    def expert(e, carry):
        pltpu.make_async_copy(wd.at[e], wd_v.at[e], wd_sem.at[e]).wait()
        d_e = dd[e].reshape(4 * cap, dim)
        da = lax.dot_general(d_e, wd_v[e], NT, preferred_element_type=F32).astype(BF16).astype(F32)
        dh1 = (da * c1_v[e]).astype(BF16)
        dh3 = (da * s_v[e]).astype(BF16)
        dh[e, :, :ffn] = dh1
        dh[e, :, ffn:] = dh3
        pltpu.make_async_copy(wg.at[e], wg_v.at[e], wg_sem.at[e]).wait()
        pltpu.make_async_copy(wu.at[e], wu_v.at[e], wu_sem.at[e]).wait()
        for n in range(0, dim, 256):
            r = lax.dot_general(dh1, wg_v[e, n:n + 256], NT, preferred_element_type=F32) + lax.dot_general(dh3, wu_v[e, n:n + 256], NT, preferred_element_type=F32)
            r = r.astype(BF16)
            for s in range(4):
                r_all[s, e, :, n:n + 256] = r[s * cap:(s + 1) * cap]
        return carry

    lax.fori_loop(0, n_loc, expert, 0)

    for i, s in enumerate((me,) + peers):
        part[i] = lax.dot_general(p_all[s], r_all[s].reshape(n_loc * cap, dim), TN, preferred_element_type=F32)

    for c in small + to_far + [to_partner] + relay:
        c.wait_send()


def weight_kernel(x, dd, aa, dh, gg, owg, owu, owd, ogg, x_v, buf_d, buf_g, buf_u, in_sem, out_sem):
    n_loc = x.shape[0]
    ffn = aa.shape[2]
    pltpu.make_async_copy(x, x_v, in_sem).start()
    ogg[...] = gg[...]

    def out_copies(e, slot):
        return (pltpu.make_async_copy(buf_d.at[slot], owd.at[e], out_sem.at[slot, 0]),
                pltpu.make_async_copy(buf_g.at[slot], owg.at[e], out_sem.at[slot, 1]),
                pltpu.make_async_copy(buf_u.at[slot], owu.at[e], out_sem.at[slot, 2]))

    def expert(e, carry):
        slot = lax.rem(e, 2)
        c_d, c_g, c_u = out_copies(e, slot)

        @pl.when(e >= 2)
        def _():
            for c in out_copies(e - 2, slot):
                c.wait()
        buf_d[slot] = lax.dot_general(aa[e], dd[e], TN, preferred_element_type=F32)
        c_d.start()

        @pl.when(e == 0)
        def _():
            pltpu.make_async_copy(x, x_v, in_sem).wait()
        buf_g[slot] = lax.dot_general(x_v[e], dh[e, :, :ffn], TN, preferred_element_type=F32)
        c_g.start()
        buf_u[slot] = lax.dot_general(x_v[e], dh[e, :, ffn:], TN, preferred_element_type=F32)
        c_u.start()
        return carry

    lax.fori_loop(0, n_loc, expert, 0)
    for e in (n_loc - 2, n_loc - 1):
        for c in out_copies(e, e % 2):
            c.wait()


def solution(mesh):
    rows_spec = P(("dp", "ep"), None)
    cube_spec = P(("dp", "ep"), None, None)
    weight_spec = P("ep", None, None)

    def local_step(grad_y, gate_vals, topk_idx, slot_ids, pair_counts, y_routed, x_disp, h_gate, h_up, w_gate, w_up, w_down):
        tok, dim = grad_y.shape
        top_k = topk_idx.shape[1]
        n_loc, _, ffn = w_gate.shape
        rows = x_disp.shape[1]
        cap = rows // 4
        n_exp = pair_counts.shape[1]
        any_spec = pl.BlockSpec(memory_space=pl.ANY)
        vmem_spec = pl.BlockSpec(memory_space=pltpu.VMEM)
        dma = pltpu.SemaphoreType.DMA
        part, dd, aa, dh, gg = pl.pallas_call(
            token_kernel,
            out_shape=(jax.ShapeDtypeStruct((4, tok, dim), F32),
                       jax.ShapeDtypeStruct((n_loc, 4, cap, dim), BF16),
                       jax.ShapeDtypeStruct((n_loc, rows, ffn), BF16),
                       jax.ShapeDtypeStruct((n_loc, rows, 2 * ffn), BF16),
                       jax.ShapeDtypeStruct((top_k, tok), F32)),
            in_specs=[any_spec] * 11,
            out_specs=(vmem_spec,) * 5,
            scratch_shapes=[
                pltpu.VMEM((4, tok, dim), BF16), pltpu.VMEM((4, top_k, tok), F32), pltpu.VMEM((4, top_k, tok), jnp.int32), pltpu.VMEM((4, top_k, tok), jnp.int32), pltpu.VMEM((4, 1, n_exp), jnp.int32),
                pltpu.VMEM((tok, top_k, dim), BF16), pltpu.VMEM((n_loc, rows, ffn), BF16), pltpu.VMEM((n_loc, rows, ffn), BF16),
                pltpu.VMEM((n_loc, dim, ffn), BF16), pltpu.VMEM((n_loc, dim, ffn), BF16), pltpu.VMEM((n_loc, ffn, dim), BF16),
                pltpu.VMEM((n_loc, rows, ffn), F32), pltpu.VMEM((n_loc, rows, ffn), F32),
                pltpu.VMEM((4, n_loc * cap, tok), BF16), pltpu.VMEM((4, n_loc, cap, dim), BF16),
                dma((5,)), dma((3,)), dma((n_loc,)), dma((n_loc,)), dma((n_loc,)),
                dma((5,)), dma((5,)), dma((3, 4)), dma((3, 4)),
            ],
            compiler_params=pltpu.CompilerParams(collective_id=0, has_side_effects=True, vmem_limit_bytes=56 * 1024 * 1024),
            cost_estimate=pl.CostEstimate(flops=4_000_000_000, bytes_accessed=30_000_000, transcendentals=0),
            name="token_kernel",
        )(grad_y, gate_vals.T, topk_idx.T, slot_ids.T, pair_counts, y_routed, h_gate, h_up, w_gate, w_up, w_down)

        pairs = ([(i, i ^ 1) for i in range(4)], [(i, i ^ 2) for i in range(4)], [(i, i ^ 3) for i in range(4)])
        got = [lax.ppermute(part[i + 1], "ep", pairs[i]) for i in (2, 1, 0)]

        owg, owu, owd, ogg = pl.pallas_call(
            weight_kernel,
            out_shape=(jax.ShapeDtypeStruct((n_loc, dim, ffn), F32),
                       jax.ShapeDtypeStruct((n_loc, dim, ffn), F32),
                       jax.ShapeDtypeStruct((n_loc, ffn, dim), F32),
                       jax.ShapeDtypeStruct((top_k, tok), F32)),
            in_specs=[any_spec] + [vmem_spec] * 4,
            out_specs=(any_spec, any_spec, any_spec, vmem_spec),
            scratch_shapes=[pltpu.VMEM((n_loc, rows, dim), BF16), pltpu.VMEM((2, ffn, dim), F32), pltpu.VMEM((2, dim, ffn), F32), pltpu.VMEM((2, dim, ffn), F32), dma(()), dma((2, 3))],
            compiler_params=pltpu.CompilerParams(vmem_limit_bytes=32 * 1024 * 1024),
            cost_estimate=pl.CostEstimate(flops=16_000_000_000, bytes_accessed=56_000_000, transcendentals=0),
            name="weight_kernel",
        )(x_disp, dd.reshape(n_loc, rows, dim), aa, dh, gg)
        grad_x = (part[0] + got[2] + got[1] + got[0]).astype(BF16)
        return grad_x, ogg.T, owg, owu, owd

    return jax.shard_map(local_step, mesh=mesh, in_specs=(rows_spec, rows_spec, rows_spec, rows_spec, rows_spec, cube_spec, cube_spec, cube_spec, cube_spec, weight_spec, weight_spec, weight_spec), out_specs=(rows_spec, rows_spec, cube_spec, cube_spec, cube_spec), check_vma=False)
```

```python
import jax
import jax.numpy as jnp
from jax import lax
from jax.experimental import pallas as pl
from jax.experimental.pallas import tpu as pltpu
from jax.sharding import PartitionSpec as P

MESH_ID = pl.DeviceIdType.MESH
F32 = jnp.float32
BF16 = jnp.bfloat16
NT = (((1,), (1,)), ((), ()))
TN = (((0,), (0,)), ((), ()))
MIB = 1024 * 1024
COLS = 256


def peer_ids():
    me = lax.axis_index("ep")
    partner = me + 1 - 2 * lax.rem(me, 2)
    return me, partner, lax.rem(me + 2, 4), lax.rem(partner + 2, 4)


def comm_kernel(gy, gv, tk, sl, pc, yr, hg, hu, wg, wu, wd,
                dd, aa, c1, act_o, p_all, wg_v, wu_v, wd_v, gg,
                gy_all, gv_all, tk_all, sl_all, pc_all, yr_v, hg_v, hu_v,
                own_sem, bulk_sem, gs_sem, gr_sem, ss_sem, sr_sem):
    n_loc = wd.shape[0]
    cap = dd.shape[2]
    tok, dim = gy.shape
    half = tok // 2
    me, partner, far, far_partner = peer_ids()
    peers = (partner, far, far_partner)

    own = [pltpu.make_async_copy(gy, gy_all.at[me], own_sem.at[0]),
           pltpu.make_async_copy(gv, gv_all.at[me], own_sem.at[1]),
           pltpu.make_async_copy(tk, tk_all.at[me], own_sem.at[2]),
           pltpu.make_async_copy(sl, sl_all.at[me], own_sem.at[3]),
           pltpu.make_async_copy(pc, pc_all.at[me], own_sem.at[4])]
    for c in own:
        c.start()
    barrier = pltpu.get_barrier_semaphore()
    for d in peers:
        pl.semaphore_signal(barrier, inc=1, device_id={"ep": d}, device_id_type=MESH_ID)
    bulk = [pltpu.make_async_copy(src, dst, bulk_sem.at[i]) for i, (src, dst) in enumerate(((hg, hg_v), (hu, hu_v), (yr, yr_v), (wd, wd_v), (wg, wg_v), (wu, wu_v)))]
    for c in bulk:
        c.start(priority=1)
    for c in own:
        c.wait()
    pl.semaphore_wait(barrier, 3)

    def remote(src, dst, ssem, rsem, dev):
        return pltpu.make_async_remote_copy(src_ref=src, dst_ref=dst, send_sem=ssem, recv_sem=rsem, device_id={"ep": dev}, device_id_type=MESH_ID)

    small = []
    for i, d in enumerate(peers):
        for k, ref in enumerate((gv_all, tk_all, sl_all, pc_all)):
            c = remote(ref.at[me], ref.at[me], ss_sem.at[i, k], sr_sem.at[i, k], d)
            c.start()
            small.append(c)
    to_far = []
    for h in range(2):
        rows = pl.ds(h * half, half)
        c = remote(gy_all.at[me, rows], gy_all.at[me, rows], gs_sem.at[1 + h], gr_sem.at[1 + h], far)
        c.start()
        to_far.append(c)
    to_partner = remote(gy_all.at[me], gy_all.at[me], gs_sem.at[0], gr_sem.at[0], partner)
    to_partner.start()

    def build(s):
        ids = tk_all[s]
        slots = sl_all[s]
        gates = gv_all[s]
        counts = pc_all[s]
        lane = lax.broadcasted_iota(jnp.int32, counts.shape, 1)
        row_c = lax.broadcasted_iota(jnp.int32, (cap, tok), 0).astype(F32)
        hots, cols = [], []
        for e in range(n_loc):
            g = me * n_loc + e
            cnt = jnp.sum(jnp.where(lane == g, counts.astype(F32), 0.0), axis=1, keepdims=True)
            slots_f = slots.astype(F32)
            ok = (ids == g) & (slots >= 0) & (slots_f < cnt)
            slot_row = jnp.max(jnp.where(ok, slots_f, -1.0), axis=0, keepdims=True)
            gate_row = jnp.sum(jnp.where(ok, gates, 0.0), axis=0, keepdims=True)
            hit = row_c == slot_row
            cols.append(jnp.sum(jnp.where(hit, gate_row, 0.0), axis=1, keepdims=True))
            hots.append(jnp.where(hit, 1.0, 0.0).astype(BF16))
        hot = jnp.concatenate(hots, axis=0)
        p_all[s] = hot
        for n in range(0, dim, COLS):
            picked = jnp.dot(hot, gy_all[s, :, n:n + COLS], preferred_element_type=F32)
            for e in range(n_loc):
                dd[e, s, :, n:n + COLS] = (picked[e * cap:(e + 1) * cap] * cols[e]).astype(BF16)

    build(me)

    bulk[0].wait()
    bulk[1].wait()

    def pre(e, carry):
        h1 = hg_v[e].astype(F32)
        h3 = hu_v[e].astype(F32)
        sig = jax.nn.sigmoid(h1)
        act = h1 * sig
        aa[e] = (act * h3).astype(BF16)
        c1[e] = h3 * sig * (1.0 + h1 * (1.0 - sig))
        act_o[e] = act
        return carry

    lax.fori_loop(0, n_loc, pre, 0)

    bulk[2].wait()
    top_k = yr.shape[1]
    dots = lax.dot_general(yr_v[...].reshape(tok * top_k, dim), gy_all[me], NT, preferred_element_type=F32).reshape(tok, top_k, tok)
    same = lax.broadcasted_iota(jnp.int32, dots.shape, 0) == lax.broadcasted_iota(jnp.int32, dots.shape, 2)
    gg[...] = jnp.sum(jnp.where(same, dots, 0.0), axis=0)

    for k in range(4):
        small[k].wait_recv()
    to_partner.wait_recv()
    build(partner)

    relay = []
    for h in range(2):
        rows = pl.ds(h * half, half)
        to_far[h].wait_recv()
        c = remote(gy_all.at[far, rows], gy_all.at[far, rows], gs_sem.at[3 + h], gr_sem.at[3 + h], partner)
        c.start()
        relay.append(c)
    for k in range(4):
        small[4 + k].wait_recv()
    build(far)
    for k in range(4):
        small[8 + k].wait_recv()
    for h in range(2):
        relay[h].wait_recv()
    build(far_partner)

    for c in bulk[3:]:
        c.wait()
    for c in small + to_far + [to_partner] + relay:
        c.wait_send()


def chain_kernel(dd, aa, c1, act, p_all, wg, wu, wd, p_own, p_partner, p_far, p_far_partner, dh, owd, r_all, buf_d, out_sem):
    n_loc, _, cap, dim = dd.shape
    ffn = aa.shape[2]
    outs = []

    def first(e):
        d_e = dd[e].reshape(4 * cap, dim)
        for n in range(0, ffn, COLS):
            da = lax.dot_general(d_e, wd[e, n:n + COLS], NT, preferred_element_type=F32).astype(BF16).astype(F32)
            dh[e, :, n:n + COLS] = (da * c1[e, :, n:n + COLS]).astype(BF16)
            dh[e, :, ffn + n:ffn + n + COLS] = (da * act[e, :, n:n + COLS]).astype(BF16)

    def second(e):
        dh1 = dh[e, :, :ffn]
        dh3 = dh[e, :, ffn:]
        for n in range(0, dim, COLS):
            r = lax.dot_general(dh1, wg[e, n:n + COLS], NT, preferred_element_type=F32) + lax.dot_general(dh3, wu[e, n:n + COLS], NT, preferred_element_type=F32)
            r = r.astype(BF16)
            for s in range(4):
                r_all[s, e, :, n:n + COLS] = r[s * cap:(s + 1) * cap]

    def down(e):
        slot = e % 2
        if e >= 2:
            outs[e - 2].wait()
        buf_d[slot] = lax.dot_general(aa[e], dd[e].reshape(4 * cap, dim), TN, preferred_element_type=F32)
        c = pltpu.make_async_copy(buf_d.at[slot], owd.at[e], out_sem.at[slot])
        c.start()
        outs.append(c)

    for e in range(n_loc):
        first(e)
        down(e)
        if e >= 1:
            second(e - 1)
    second(n_loc - 1)

    me, partner, far, far_partner = peer_ids()
    for s, ref in ((me, p_own), (partner, p_partner), (far, p_far), (far_partner, p_far_partner)):
        ref[...] = lax.dot_general(p_all[s], r_all[s].reshape(n_loc * cap, dim), TN, preferred_element_type=F32)
    for c in outs[-2:]:
        c.wait()


def weight_kernel(x, dh, gg, owg, owu, ogg, buf_g, buf_u, out_sem):
    n_loc = x.shape[0]
    ffn = owg.shape[2]
    ogg[...] = gg[...]

    def out_copies(e, slot):
        return (pltpu.make_async_copy(buf_g.at[slot], owg.at[e], out_sem.at[slot, 0]),
                pltpu.make_async_copy(buf_u.at[slot], owu.at[e], out_sem.at[slot, 1]))

    def expert(e, carry):
        slot = lax.rem(e, 2)
        c_g, c_u = out_copies(e, slot)

        @pl.when(e >= 2)
        def _():
            for c in out_copies(e - 2, slot):
                c.wait()
        buf_g[slot] = lax.dot_general(x[e], dh[e, :, :ffn], TN, preferred_element_type=F32)
        c_g.start()
        buf_u[slot] = lax.dot_general(x[e], dh[e, :, ffn:], TN, preferred_element_type=F32)
        c_u.start()
        return carry

    lax.fori_loop(0, n_loc, expert, 0)
    for e in (n_loc - 2, n_loc - 1):
        for c in out_copies(e, e % 2):
            c.wait()


def solution(mesh):
    rows_spec = P(("dp", "ep"), None)
    cube_spec = P(("dp", "ep"), None, None)
    weight_spec = P("ep", None, None)

    def local_step(grad_y, gate_vals, topk_idx, slot_ids, pair_counts, y_routed, x_disp, h_gate, h_up, w_gate, w_up, w_down):
        tok, dim = grad_y.shape
        top_k = topk_idx.shape[1]
        n_loc, _, ffn = w_gate.shape
        rows = x_disp.shape[1]
        cap = rows // 4
        n_exp = pair_counts.shape[1]
        hbm_spec = pl.BlockSpec(memory_space=pltpu.HBM)
        any_spec = pl.BlockSpec(memory_space=pl.ANY)
        vmem_spec = pl.BlockSpec(memory_space=pltpu.VMEM)
        dma = pltpu.SemaphoreType.DMA
        shape = jax.ShapeDtypeStruct
        ins = [pltpu.with_memory_space_constraint(a, pltpu.HBM) for a in (grad_y, gate_vals.T, topk_idx.T, slot_ids.T, pair_counts, y_routed, h_gate, h_up, w_gate, w_up, w_down)]
        dd, aa, c1, act, p_all, wg_v, wu_v, wd_v, gg = pl.pallas_call(
            comm_kernel,
            out_shape=(shape((n_loc, 4, cap, dim), BF16), shape((n_loc, rows, ffn), BF16), shape((n_loc, rows, ffn), F32), shape((n_loc, rows, ffn), F32),
                       shape((4, n_loc * cap, tok), BF16), shape(w_gate.shape, BF16), shape(w_up.shape, BF16), shape(w_down.shape, BF16), shape((top_k, tok), F32)),
            in_specs=[hbm_spec] * 11,
            out_specs=(vmem_spec,) * 9,
            scratch_shapes=[
                pltpu.VMEM((4, tok, dim), BF16), pltpu.VMEM((4, top_k, tok), F32), pltpu.VMEM((4, top_k, tok), jnp.int32), pltpu.VMEM((4, top_k, tok), jnp.int32), pltpu.VMEM((4, 1, n_exp), jnp.int32),
                pltpu.VMEM((tok, top_k, dim), BF16), pltpu.VMEM((n_loc, rows, ffn), BF16), pltpu.VMEM((n_loc, rows, ffn), BF16),
                dma((5,)), dma((6,)), dma((5,)), dma((5,)), dma((3, 4)), dma((3, 4)),
            ],
            compiler_params=pltpu.CompilerParams(collective_id=0, has_side_effects=True, vmem_limit_bytes=8 * MIB),
            cost_estimate=pl.CostEstimate(flops=1_000_000_000, bytes_accessed=30_000_000, transcendentals=0),
            name="comm_kernel",
        )(*ins)

        p_own, p_partner, p_far, p_far_partner, dh, owd = pl.pallas_call(
            chain_kernel,
            out_shape=(shape((tok, dim), F32),) * 4 + (shape((n_loc, rows, 2 * ffn), BF16), shape((n_loc, ffn, dim), F32)),
            in_specs=[vmem_spec] * 8,
            out_specs=(vmem_spec,) * 5 + (hbm_spec,),
            scratch_shapes=[pltpu.VMEM((4, n_loc, cap, dim), BF16), pltpu.VMEM((2, ffn, dim), F32), dma((2,))],
            compiler_params=pltpu.CompilerParams(vmem_limit_bytes=12 * MIB),
            cost_estimate=pl.CostEstimate(flops=4_000_000_000, bytes_accessed=20_000_000, transcendentals=0),
            name="chain_kernel",
        )(dd, aa, c1, act, p_all, wg_v, wu_v, wd_v)

        pairs = [[(i, i ^ k) for i in range(4)] for k in (1, 2, 3)]
        got_fp = lax.ppermute(p_far_partner, "ep", pairs[2])
        got_f = lax.ppermute(p_far, "ep", pairs[1])
        got_p = lax.ppermute(p_partner, "ep", pairs[0])

        owg, owu, ogg = pl.pallas_call(
            weight_kernel,
            out_shape=(shape((n_loc, dim, ffn), F32), shape((n_loc, dim, ffn), F32), shape((top_k, tok), F32)),
            in_specs=[vmem_spec] * 3,
            out_specs=(hbm_spec, hbm_spec, vmem_spec),
            scratch_shapes=[pltpu.VMEM((2, dim, ffn), F32), pltpu.VMEM((2, dim, ffn), F32), dma((2, 2))],
            compiler_params=pltpu.CompilerParams(vmem_limit_bytes=16 * MIB),
            cost_estimate=pl.CostEstimate(flops=16_000_000_000, bytes_accessed=56_000_000, transcendentals=0),
            name="weight_kernel",
        )(x_disp, dh, gg)
        grad_x = (p_own + got_p + got_f + got_fp).astype(BF16)
        return grad_x, ogg.T, owg, owu, owd

    return jax.shard_map(local_step, mesh=mesh, in_specs=(rows_spec, rows_spec, rows_spec, rows_spec, rows_spec, cube_spec, cube_spec, cube_spec, cube_spec, weight_spec, weight_spec, weight_spec), out_specs=(rows_spec, rows_spec, cube_spec, cube_spec, cube_spec), check_vma=False)
```

```python
import jax
import jax.numpy as jnp
from jax import lax
from jax.experimental import pallas as pl
from jax.experimental.pallas import tpu as pltpu
from jax.sharding import PartitionSpec as P

MESH_ID = pl.DeviceIdType.MESH
F32 = jnp.float32
BF16 = jnp.bfloat16
NT = (((1,), (1,)), ((), ()))
TN = (((0,), (0,)), ((), ()))
MIB = 1024 * 1024
COLS = 256
LATE = 2


def peer_ids():
    me = lax.axis_index("ep")
    partner = me + 1 - 2 * lax.rem(me, 2)
    return me, partner, lax.rem(me + 2, 4), lax.rem(partner + 2, 4)


def comm_kernel(gy, gv, tk, sl, pc, yr, hg, hu, wg, wu, wd,
                dd, aa, c1, act_o, p_all, wg_v, wu_v, wd_v, gg,
                gy_all, gv_all, tk_all, sl_all, pc_all, yr_v, hg_v, hu_v,
                own_sem, bulk_sem, gs_sem, gr_sem, ss_sem, sr_sem):
    n_loc = wd.shape[0]
    cap = dd.shape[2]
    tok, dim = gy.shape
    half = tok // 2
    early = wg_v.shape[0]
    me, partner, far, far_partner = peer_ids()
    peers = (partner, far, far_partner)

    own = [pltpu.make_async_copy(gy, gy_all.at[me], own_sem.at[0]),
           pltpu.make_async_copy(gv, gv_all.at[me], own_sem.at[1]),
           pltpu.make_async_copy(tk, tk_all.at[me], own_sem.at[2]),
           pltpu.make_async_copy(sl, sl_all.at[me], own_sem.at[3]),
           pltpu.make_async_copy(pc, pc_all.at[me], own_sem.at[4])]
    for c in own:
        c.start()
    barrier = pltpu.get_barrier_semaphore()
    for d in peers:
        pl.semaphore_signal(barrier, inc=1, device_id={"ep": d}, device_id_type=MESH_ID)
    bulk = [pltpu.make_async_copy(src, dst, bulk_sem.at[i]) for i, (src, dst) in enumerate(((hg, hg_v), (hu, hu_v), (yr, yr_v), (wd, wd_v), (wg.at[pl.ds(0, early)], wg_v), (wu.at[pl.ds(0, early)], wu_v)))]
    for c in bulk:
        c.start(priority=1)
    for c in own:
        c.wait()
    pl.semaphore_wait(barrier, 3)

    def remote(src, dst, ssem, rsem, dev):
        return pltpu.make_async_remote_copy(src_ref=src, dst_ref=dst, send_sem=ssem, recv_sem=rsem, device_id={"ep": dev}, device_id_type=MESH_ID)

    small = []
    to_far = []
    to_partner = remote(gy_all.at[me], gy_all.at[me], gs_sem.at[0], gr_sem.at[0], partner)
    for h in range(2):
        rows = pl.ds(h * half, half)
        to_far.append(remote(gy_all.at[me, rows], gy_all.at[me, rows], gs_sem.at[1 + h], gr_sem.at[1 + h], far))
    for i, d in enumerate(peers):
        for k, ref in enumerate((gv_all, tk_all, sl_all, pc_all)):
            small.append(remote(ref.at[me], ref.at[me], ss_sem.at[i, k], sr_sem.at[i, k], d))
    for c in to_far + small + [to_partner]:
        c.start()

    def build(s):
        ids = tk_all[s]
        slots = sl_all[s]
        gates = gv_all[s]
        counts = pc_all[s]
        lane = lax.broadcasted_iota(jnp.int32, counts.shape, 1)
        row_c = lax.broadcasted_iota(jnp.int32, (cap, tok), 0).astype(F32)
        hots, cols = [], []
        for e in range(n_loc):
            g = me * n_loc + e
            cnt = jnp.sum(jnp.where(lane == g, counts.astype(F32), 0.0), axis=1, keepdims=True)
            slots_f = slots.astype(F32)
            ok = (ids == g) & (slots >= 0) & (slots_f < cnt)
            slot_row = jnp.max(jnp.where(ok, slots_f, -1.0), axis=0, keepdims=True)
            gate_row = jnp.sum(jnp.where(ok, gates, 0.0), axis=0, keepdims=True)
            hit = row_c == slot_row
            cols.append(jnp.sum(jnp.where(hit, gate_row, 0.0), axis=1, keepdims=True))
            hots.append(jnp.where(hit, 1.0, 0.0).astype(BF16))
        hot = jnp.concatenate(hots, axis=0)
        p_all[s] = hot
        for n in range(0, dim, COLS):
            picked = jnp.dot(hot, gy_all[s, :, n:n + COLS], preferred_element_type=F32)
            for e in range(n_loc):
                dd[e, s, :, n:n + COLS] = (picked[e * cap:(e + 1) * cap] * cols[e]).astype(BF16)

    build(me)

    bulk[0].wait()
    bulk[1].wait()

    def pre(e, carry):
        h1 = hg_v[e].astype(F32)
        h3 = hu_v[e].astype(F32)
        sig = jax.nn.sigmoid(h1)
        act = h1 * sig
        aa[e] = (act * h3).astype(BF16)
        c1[e] = h3 * sig * (1.0 + h1 * (1.0 - sig))
        act_o[e] = act
        return carry

    lax.fori_loop(0, n_loc, pre, 0)

    bulk[2].wait()
    top_k = yr.shape[1]
    dots = lax.dot_general(yr_v[...].reshape(tok * top_k, dim), gy_all[me], NT, preferred_element_type=F32).reshape(tok, top_k, tok)
    same = lax.broadcasted_iota(jnp.int32, dots.shape, 0) == lax.broadcasted_iota(jnp.int32, dots.shape, 2)
    gg[...] = jnp.sum(jnp.where(same, dots, 0.0), axis=0)

    for k in range(4):
        small[k].wait_recv()
    to_partner.wait_recv()
    build(partner)

    relay = []
    for h in range(2):
        rows = pl.ds(h * half, half)
        to_far[h].wait_recv()
        c = remote(gy_all.at[far, rows], gy_all.at[far, rows], gs_sem.at[3 + h], gr_sem.at[3 + h], partner)
        c.start()
        relay.append(c)
    for k in range(4):
        small[4 + k].wait_recv()
    build(far)
    for k in range(4):
        small[8 + k].wait_recv()
    for h in range(2):
        relay[h].wait_recv()
    build(far_partner)

    for c in bulk[3:]:
        c.wait()
    for c in small + to_far + [to_partner] + relay:
        c.wait_send()


def mix(main, side):
    done = 0
    for k, work in enumerate(main):
        work()
        upto = len(side) * (k + 1) // len(main)
        for extra in side[done:upto]:
            extra()
        done = upto


def chain_kernel(dd, aa, c1, act, p_all, wg, wu, wd, wg_hbm, wu_hbm, p_own, p_partner, p_far, p_far_partner, dh, owd, r_all, buf_d, wg_l, wu_l, out_sem, in_sem):
    n_loc, _, cap, dim = dd.shape
    ffn = aa.shape[2]
    early = wg.shape[0]
    pairs = n_loc // 2
    ins = [pltpu.make_async_copy(wg_hbm.at[pl.ds(early, LATE)], wg_l, in_sem.at[0]), pltpu.make_async_copy(wu_hbm.at[pl.ds(early, LATE)], wu_l, in_sem.at[1])]
    for c in ins:
        c.start()

    def first(e, n):
        def work():
            da = lax.dot_general(dd[e].reshape(4 * cap, dim), wd[e, n:n + COLS], NT, preferred_element_type=F32).astype(BF16).astype(F32)
            dh[e, :, n:n + COLS] = (da * c1[e, :, n:n + COLS]).astype(BF16)
            dh[e, :, ffn + n:ffn + n + COLS] = (da * act[e, :, n:n + COLS]).astype(BF16)
        return work

    def second(e, n):
        def work():
            g, u = (wg[e, n:n + COLS], wu[e, n:n + COLS]) if e < early else (wg_l[e - early, n:n + COLS], wu_l[e - early, n:n + COLS])
            r = lax.dot_general(dh[e, :, :ffn], g, NT, preferred_element_type=F32) + lax.dot_general(dh[e, :, ffn:], u, NT, preferred_element_type=F32)
            r = r.astype(BF16)
            for s in range(4):
                r_all[s, e, :, n:n + COLS] = r[s * cap:(s + 1) * cap]
        return work

    def down(e, n, m):
        def work():
            buf_d[(e // 2) % 2, e % 2, m:m + COLS, n:n + COLS] = lax.dot_general(aa[e, :, m:m + COLS], dd[e, :, :, n:n + COLS].reshape(4 * cap, COLS), TN, preferred_element_type=F32)
        return work

    outs = [pltpu.make_async_copy(buf_d.at[p % 2], owd.at[pl.ds(2 * p, 2)], out_sem.at[p % 2]) for p in range(pairs)]
    for p in range(-1, pairs):
        main, side = [], []
        if p >= 0:
            main += [second(2 * p + i, n) for n in range(0, dim, COLS) for i in range(2)]
        if p + 1 < pairs:
            main += [first(2 * p + 2 + i, n) for n in range(0, ffn, COLS) for i in range(2)]
            side += [down(2 * p + 2 + i, n, m) for i in range(2) for n in range(0, dim, COLS) for m in range(0, ffn, COLS)]
            if p >= 1:
                outs[p - 1].wait()
        else:
            for c in ins:
                c.wait()
        mix(main, side)
        if p + 1 < pairs:
            outs[p + 1].start()

    me, partner, far, far_partner = peer_ids()
    for s, ref in ((me, p_own), (partner, p_partner), (far, p_far), (far_partner, p_far_partner)):
        ref[...] = lax.dot_general(p_all[s], r_all[s].reshape(n_loc * cap, dim), TN, preferred_element_type=F32)
    for c in outs[-2:]:
        c.wait()


def weight_kernel(x, dh, gg, owg, owu, ogg, buf_g, buf_u, out_sem):
    n_loc = x.shape[0]
    ffn = owg.shape[2]
    ogg[...] = gg[...]

    def out_copies(e, slot):
        return (pltpu.make_async_copy(buf_g.at[slot], owg.at[e], out_sem.at[slot, 0]),
                pltpu.make_async_copy(buf_u.at[slot], owu.at[e], out_sem.at[slot, 1]))

    def expert(e, carry):
        slot = lax.rem(e, 2)
        c_g, c_u = out_copies(e, slot)

        @pl.when(e >= 2)
        def _():
            for c in out_copies(e - 2, slot):
                c.wait()
        buf_g[slot] = lax.dot_general(x[e], dh[e, :, :ffn], TN, preferred_element_type=F32)
        c_g.start()
        buf_u[slot] = lax.dot_general(x[e], dh[e, :, ffn:], TN, preferred_element_type=F32)
        c_u.start()
        return carry

    lax.fori_loop(0, n_loc, expert, 0)
    for e in (n_loc - 2, n_loc - 1):
        for c in out_copies(e, e % 2):
            c.wait()


def solution(mesh):
    rows_spec = P(("dp", "ep"), None)
    cube_spec = P(("dp", "ep"), None, None)
    weight_spec = P("ep", None, None)

    def local_step(grad_y, gate_vals, topk_idx, slot_ids, pair_counts, y_routed, x_disp, h_gate, h_up, w_gate, w_up, w_down):
        tok, dim = grad_y.shape
        top_k = topk_idx.shape[1]
        n_loc, _, ffn = w_gate.shape
        rows = x_disp.shape[1]
        cap = rows // 4
        n_exp = pair_counts.shape[1]
        hbm_spec = pl.BlockSpec(memory_space=pltpu.HBM)
        any_spec = pl.BlockSpec(memory_space=pl.ANY)
        vmem_spec = pl.BlockSpec(memory_space=pltpu.VMEM)
        dma = pltpu.SemaphoreType.DMA
        shape = jax.ShapeDtypeStruct
        ins = [pltpu.with_memory_space_constraint(a, pltpu.HBM) for a in (grad_y, gate_vals.T, topk_idx.T, slot_ids.T, pair_counts, y_routed, h_gate, h_up, w_gate, w_up, w_down)]
        dd, aa, c1, act, p_all, wg_v, wu_v, wd_v, gg = pl.pallas_call(
            comm_kernel,
            out_shape=(shape((n_loc, 4, cap, dim), BF16), shape((n_loc, rows, ffn), BF16), shape((n_loc, rows, ffn), F32), shape((n_loc, rows, ffn), F32),
                       shape((4, n_loc * cap, tok), BF16), shape((n_loc - LATE, dim, ffn), BF16), shape((n_loc - LATE, dim, ffn), BF16), shape(w_down.shape, BF16), shape((top_k, tok), F32)),
            in_specs=[hbm_spec] * 11,
            out_specs=(vmem_spec,) * 9,
            scratch_shapes=[
                pltpu.VMEM((4, tok, dim), BF16), pltpu.VMEM((4, top_k, tok), F32), pltpu.VMEM((4, top_k, tok), jnp.int32), pltpu.VMEM((4, top_k, tok), jnp.int32), pltpu.VMEM((4, 1, n_exp), jnp.int32),
                pltpu.VMEM((tok, top_k, dim), BF16), pltpu.VMEM((n_loc, rows, ffn), BF16), pltpu.VMEM((n_loc, rows, ffn), BF16),
                dma((5,)), dma((6,)), dma((5,)), dma((5,)), dma((3, 4)), dma((3, 4)),
            ],
            compiler_params=pltpu.CompilerParams(collective_id=0, has_side_effects=True, vmem_limit_bytes=8 * MIB),
            cost_estimate=pl.CostEstimate(flops=1_000_000_000, bytes_accessed=30_000_000, transcendentals=0),
            name="comm_kernel",
        )(*ins)

        p_own, p_partner, p_far, p_far_partner, dh, owd = pl.pallas_call(
            chain_kernel,
            out_shape=(shape((tok, dim), F32),) * 4 + (shape((n_loc, rows, 2 * ffn), BF16), shape((n_loc, ffn, dim), F32)),
            in_specs=[vmem_spec] * 8 + [hbm_spec] * 2,
            out_specs=(vmem_spec,) * 5 + (hbm_spec,),
            scratch_shapes=[pltpu.VMEM((4, n_loc, cap, dim), BF16), pltpu.VMEM((2, 2, ffn, dim), F32), pltpu.VMEM((LATE, dim, ffn), BF16), pltpu.VMEM((LATE, dim, ffn), BF16), dma((2,)), dma((2,))],
            compiler_params=pltpu.CompilerParams(vmem_limit_bytes=18 * MIB),
            cost_estimate=pl.CostEstimate(flops=4_000_000_000, bytes_accessed=20_000_000, transcendentals=0),
            name="chain_kernel",
        )(dd, aa, c1, act, p_all, wg_v, wu_v, wd_v, ins[8], ins[9])

        pairs = [[(i, i ^ k) for i in range(4)] for k in (1, 2, 3)]
        got_fp = lax.ppermute(p_far_partner, "ep", pairs[2])
        got_f = lax.ppermute(p_far, "ep", pairs[1])
        got_p = lax.ppermute(p_partner, "ep", pairs[0])

        owg, owu, ogg = pl.pallas_call(
            weight_kernel,
            out_shape=(shape((n_loc, dim, ffn), F32), shape((n_loc, dim, ffn), F32), shape((top_k, tok), F32)),
            in_specs=[vmem_spec] * 3,
            out_specs=(hbm_spec, hbm_spec, vmem_spec),
            scratch_shapes=[pltpu.VMEM((2, dim, ffn), F32), pltpu.VMEM((2, dim, ffn), F32), dma((2, 2))],
            compiler_params=pltpu.CompilerParams(vmem_limit_bytes=16 * MIB),
            cost_estimate=pl.CostEstimate(flops=16_000_000_000, bytes_accessed=56_000_000, transcendentals=0),
            name="weight_kernel",
        )(x_disp, dh, gg)
        grad_x = (p_own + got_p + got_f + got_fp).astype(BF16)
        return grad_x, ogg.T, owg, owu, owd

    return jax.shard_map(local_step, mesh=mesh, in_specs=(rows_spec, rows_spec, rows_spec, rows_spec, rows_spec, cube_spec, cube_spec, cube_spec, cube_spec, weight_spec, weight_spec, weight_spec), out_specs=(rows_spec, rows_spec, cube_spec, cube_spec, cube_spec), check_vma=False)
```

```python
import jax
import jax.numpy as jnp
from jax import lax
from jax.experimental import pallas as pl
from jax.experimental.pallas import tpu as pltpu
from jax.sharding import PartitionSpec as P

MESH_ID = pl.DeviceIdType.MESH
F32 = jnp.float32
BF16 = jnp.bfloat16
NT = (((1,), (1,)), ((), ()))
TN = (((0,), (0,)), ((), ()))
MIB = 1024 * 1024
COLS = 256
LATE = 2


def peer_ids():
    me = lax.axis_index("ep")
    partner = me + 1 - 2 * lax.rem(me, 2)
    return me, partner, lax.rem(me + 2, 4), lax.rem(partner + 2, 4)


def comm_kernel(gy, gv, tk, sl, pc, yr, hg, hu, wg, wu, wd,
                dd, aa, c1, act_o, p_all, wg_v, wu_v, wd_v, gg,
                gy_all, gv_all, tk_all, sl_all, pc_all, yr_v, hg_v, hu_v,
                own_sem, bulk_sem, gs_sem, gr_sem, ss_sem, sr_sem):
    n_loc = wd.shape[0]
    cap = dd.shape[2]
    tok, dim = gy.shape
    half = tok // 2
    early = wg_v.shape[0]
    me, partner, far, far_partner = peer_ids()
    peers = (partner, far, far_partner)

    own = [pltpu.make_async_copy(gy, gy_all.at[me], own_sem.at[0]),
           pltpu.make_async_copy(gv, gv_all.at[me], own_sem.at[1]),
           pltpu.make_async_copy(tk, tk_all.at[me], own_sem.at[2]),
           pltpu.make_async_copy(sl, sl_all.at[me], own_sem.at[3]),
           pltpu.make_async_copy(pc, pc_all.at[me], own_sem.at[4])]
    for c in own:
        c.start()
    barrier = pltpu.get_barrier_semaphore()
    for d in peers:
        pl.semaphore_signal(barrier, inc=1, device_id={"ep": d}, device_id_type=MESH_ID)
    bulk = [pltpu.make_async_copy(src, dst, bulk_sem.at[i]) for i, (src, dst) in enumerate(((hg, hg_v), (hu, hu_v), (yr, yr_v), (wd, wd_v), (wg.at[pl.ds(0, early)], wg_v), (wu.at[pl.ds(0, early)], wu_v)))]
    for c in bulk:
        c.start(priority=1)
    for c in own:
        c.wait()
    pl.semaphore_wait(barrier, 3)

    def remote(src, dst, ssem, rsem, dev):
        return pltpu.make_async_remote_copy(src_ref=src, dst_ref=dst, send_sem=ssem, recv_sem=rsem, device_id={"ep": dev}, device_id_type=MESH_ID)

    small = []
    to_far = []
    to_partner = remote(gy_all.at[me], gy_all.at[me], gs_sem.at[0], gr_sem.at[0], partner)
    for h in range(2):
        rows = pl.ds(h * half, half)
        to_far.append(remote(gy_all.at[me, rows], gy_all.at[me, rows], gs_sem.at[1 + h], gr_sem.at[1 + h], far))
    for i, d in enumerate(peers):
        for k, ref in enumerate((gv_all, tk_all, sl_all, pc_all)):
            small.append(remote(ref.at[me], ref.at[me], ss_sem.at[i, k], sr_sem.at[i, k], d))
    for c in to_far + small + [to_partner]:
        c.start()

    def build(s):
        ids = tk_all[s]
        slots = sl_all[s]
        gates = gv_all[s]
        counts = pc_all[s]
        lane = lax.broadcasted_iota(jnp.int32, counts.shape, 1)
        row_c = lax.broadcasted_iota(jnp.int32, (cap, tok), 0).astype(F32)
        hots, cols = [], []
        for e in range(n_loc):
            g = me * n_loc + e
            cnt = jnp.sum(jnp.where(lane == g, counts.astype(F32), 0.0), axis=1, keepdims=True)
            slots_f = slots.astype(F32)
            ok = (ids == g) & (slots >= 0) & (slots_f < cnt)
            slot_row = jnp.max(jnp.where(ok, slots_f, -1.0), axis=0, keepdims=True)
            gate_row = jnp.sum(jnp.where(ok, gates, 0.0), axis=0, keepdims=True)
            hit = row_c == slot_row
            cols.append(jnp.sum(jnp.where(hit, gate_row, 0.0), axis=1, keepdims=True))
            hots.append(jnp.where(hit, 1.0, 0.0).astype(BF16))
        hot = jnp.concatenate(hots, axis=0)
        p_all[s] = hot.astype(F32).T.astype(BF16)
        for n in range(0, dim, COLS):
            picked = jnp.dot(hot, gy_all[s, :, n:n + COLS], preferred_element_type=F32)
            for e in range(n_loc):
                dd[e, s, :, n:n + COLS] = (picked[e * cap:(e + 1) * cap] * cols[e]).astype(BF16)

    build(me)

    bulk[0].wait()
    bulk[1].wait()

    def pre(e, carry):
        h1 = hg_v[e].astype(F32)
        h3 = hu_v[e].astype(F32)
        sig = jax.nn.sigmoid(h1)
        act = h1 * sig
        aa[e] = (act * h3).T.astype(BF16)
        c1[e] = h3 * sig * (1.0 + h1 * (1.0 - sig))
        act_o[e] = act
        return carry

    lax.fori_loop(0, n_loc, pre, 0)

    bulk[2].wait()
    top_k = yr.shape[1]
    dots = lax.dot_general(yr_v[...].reshape(tok * top_k, dim), gy_all[me], NT, preferred_element_type=F32).reshape(tok, top_k, tok)
    same = lax.broadcasted_iota(jnp.int32, dots.shape, 0) == lax.broadcasted_iota(jnp.int32, dots.shape, 2)
    gg[...] = jnp.sum(jnp.where(same, dots, 0.0), axis=0)

    for k in range(4):
        small[k].wait_recv()
    to_partner.wait_recv()
    build(partner)

    relay = []
    for h in range(2):
        rows = pl.ds(h * half, half)
        to_far[h].wait_recv()
        c = remote(gy_all.at[far, rows], gy_all.at[far, rows], gs_sem.at[3 + h], gr_sem.at[3 + h], partner)
        c.start()
        relay.append(c)
    for k in range(4):
        small[4 + k].wait_recv()
    build(far)
    for k in range(4):
        small[8 + k].wait_recv()
    for h in range(2):
        relay[h].wait_recv()
    build(far_partner)

    for c in bulk[3:]:
        c.wait()
    for c in small + to_far + [to_partner] + relay:
        c.wait_send()


def chain_kernel(dd, aa, c1, act, p_all, wg, wu, wd, wg_hbm, wu_hbm, p_own, p_partner, p_far, p_far_partner, dh, owd, r_all, buf_d, wg_l, wu_l, out_sem, in_sem, tail_sem):
    n_loc, _, cap, dim = dd.shape
    ffn = aa.shape[1]
    early = wg.shape[0]
    pairs = n_loc // 2
    ins = [pltpu.make_async_copy(wg_hbm.at[pl.ds(early, LATE)], wg_l, in_sem.at[0]), pltpu.make_async_copy(wu_hbm.at[pl.ds(early, LATE)], wu_l, in_sem.at[1])]
    for c in ins:
        c.start()

    def first(ea, eb, n, side):
        acc = [None] * 2
        for k in range(0, dim, COLS):
            terms = [lax.dot_general(dd[e, :, :, k:k + COLS].reshape(4 * cap, COLS), wd[e, n:n + COLS, k:k + COLS], NT, preferred_element_type=F32) for e in (ea, eb)]
            acc = [x if a is None else a + x for a, x in zip(acc, terms)]
            for work in side[k // COLS]:
                work()
        for e, da in zip((ea, eb), acc):
            da = da.astype(BF16).astype(F32)
            dh[e, :, n:n + COLS] = (da * c1[e, :, n:n + COLS]).astype(BF16)
            dh[e, :, ffn + n:ffn + n + COLS] = (da * act[e, :, n:n + COLS]).astype(BF16)

    def gate_up_weight(e, n, k):
        ref = (wg, wu) if e < early else (wg_l, wu_l)
        return ref[k // ffn][e if e < early else e - early, n:n + COLS, k % ffn:k % ffn + COLS]

    def second(ea, eb, na, nb):
        acc = [None] * 4
        for k in range(0, 2 * ffn, COLS):
            terms = [lax.dot_general(dh[ea, :, k:k + COLS], gate_up_weight(ea, n, k), NT, preferred_element_type=F32) for n in (na, nb)]
            terms += [lax.dot_general(gate_up_weight(eb, n, k), dh[eb, :, k:k + COLS], NT, preferred_element_type=F32) for n in (na, nb)]
            acc = [x if a is None else a + x for a, x in zip(acc, terms)]
        for i, n in enumerate((na, nb)):
            ra = acc[i].astype(BF16)
            rb = acc[2 + i].astype(BF16).T
            for s in range(4):
                r_all[s, ea, :, n:n + COLS] = ra[s * cap:(s + 1) * cap]
                r_all[s, eb, :, n:n + COLS] = rb[s * cap:(s + 1) * cap]

    def down(e, n, m):
        def work():
            buf_d[(e // 2) % 2, e % 2, m:m + COLS, n:n + COLS] = jnp.dot(aa[e, m:m + COLS], dd[e, :, :, n:n + COLS].reshape(4 * cap, COLS), preferred_element_type=F32)
        return work

    outs = [pltpu.make_async_copy(buf_d.at[p % 2], owd.at[pl.ds(2 * p, 2)], out_sem.at[p % 2]) for p in range(pairs - 1)]
    tail = [pltpu.make_async_copy(buf_d.at[(pairs - 1) % 2, i], owd.at[n_loc - 2 + i], tail_sem.at[i]) for i in range(2)]
    for p in range(-1, pairs):
        ea, eb = 2 * p, 2 * p + 1
        if 1 <= p < pairs - 1:
            outs[p - 1].wait()
        if p == pairs - 1:
            for c in ins:
                c.wait()
        if p >= 0:
            for n in range(0, dim, 2 * COLS):
                second(ea, eb, n, n + COLS)
        if p + 1 < pairs:
            side = [down(ea + 2 + i, n, m) for i in range(2) for n in range(0, dim, COLS) for m in range(0, ffn, COLS)]
            for h, n in enumerate(range(0, ffn, COLS)):
                first(ea + 2, eb + 2, n, [side[8 * h + 2 * q:8 * h + 2 * q + 2] for q in range(4)])
                if p + 2 == pairs:
                    tail[h].start()
            if p + 2 < pairs:
                outs[p + 1].start()

    me, partner, far, far_partner = peer_ids()
    for s, ref in ((me, p_own), (partner, p_partner), (far, p_far), (far_partner, p_far_partner)):
        ref[...] = jnp.dot(p_all[s], r_all[s].reshape(n_loc * cap, dim), preferred_element_type=F32)
    for c in outs[-1:] + tail:
        c.wait()


def weight_kernel(x, dh, gg, owg, owu, ogg, buf_g, buf_u, out_sem):
    n_loc = x.shape[0]
    ffn = owg.shape[2]
    ogg[...] = gg[...]

    def out_copies(e, slot):
        return (pltpu.make_async_copy(buf_g.at[slot], owg.at[e], out_sem.at[slot, 0]),
                pltpu.make_async_copy(buf_u.at[slot], owu.at[e], out_sem.at[slot, 1]))

    def expert(e, carry):
        slot = lax.rem(e, 2)
        c_g, c_u = out_copies(e, slot)

        @pl.when(e >= 2)
        def _():
            for c in out_copies(e - 2, slot):
                c.wait()
        buf_g[slot] = lax.dot_general(x[e], dh[e, :, :ffn], TN, preferred_element_type=F32)
        c_g.start()
        buf_u[slot] = lax.dot_general(x[e], dh[e, :, ffn:], TN, preferred_element_type=F32)
        c_u.start()
        return carry

    lax.fori_loop(0, n_loc, expert, 0)
    for e in (n_loc - 2, n_loc - 1):
        for c in out_copies(e, e % 2):
            c.wait()


def solution(mesh):
    rows_spec = P(("dp", "ep"), None)
    cube_spec = P(("dp", "ep"), None, None)
    weight_spec = P("ep", None, None)

    def local_step(grad_y, gate_vals, topk_idx, slot_ids, pair_counts, y_routed, x_disp, h_gate, h_up, w_gate, w_up, w_down):
        tok, dim = grad_y.shape
        top_k = topk_idx.shape[1]
        n_loc, _, ffn = w_gate.shape
        rows = x_disp.shape[1]
        cap = rows // 4
        n_exp = pair_counts.shape[1]
        hbm_spec = pl.BlockSpec(memory_space=pltpu.HBM)
        any_spec = pl.BlockSpec(memory_space=pl.ANY)
        vmem_spec = pl.BlockSpec(memory_space=pltpu.VMEM)
        dma = pltpu.SemaphoreType.DMA
        shape = jax.ShapeDtypeStruct
        ins = [pltpu.with_memory_space_constraint(a, pltpu.HBM) for a in (grad_y, gate_vals.T, topk_idx.T, slot_ids.T, pair_counts, y_routed, h_gate, h_up, w_gate, w_up, w_down)]
        dd, aa, c1, act, p_all, wg_v, wu_v, wd_v, gg = pl.pallas_call(
            comm_kernel,
            out_shape=(shape((n_loc, 4, cap, dim), BF16), shape((n_loc, ffn, rows), BF16), shape((n_loc, rows, ffn), F32), shape((n_loc, rows, ffn), F32),
                       shape((4, tok, n_loc * cap), BF16), shape((n_loc - LATE, dim, ffn), BF16), shape((n_loc - LATE, dim, ffn), BF16), shape(w_down.shape, BF16), shape((top_k, tok), F32)),
            in_specs=[hbm_spec] * 11,
            out_specs=(vmem_spec,) * 9,
            scratch_shapes=[
                pltpu.VMEM((4, tok, dim), BF16), pltpu.VMEM((4, top_k, tok), F32), pltpu.VMEM((4, top_k, tok), jnp.int32), pltpu.VMEM((4, top_k, tok), jnp.int32), pltpu.VMEM((4, 1, n_exp), jnp.int32),
                pltpu.VMEM((tok, top_k, dim), BF16), pltpu.VMEM((n_loc, rows, ffn), BF16), pltpu.VMEM((n_loc, rows, ffn), BF16),
                dma((5,)), dma((6,)), dma((5,)), dma((5,)), dma((3, 4)), dma((3, 4)),
            ],
            compiler_params=pltpu.CompilerParams(collective_id=0, has_side_effects=True, vmem_limit_bytes=8 * MIB),
            cost_estimate=pl.CostEstimate(flops=1_000_000_000, bytes_accessed=30_000_000, transcendentals=0),
            name="comm_kernel",
        )(*ins)

        p_own, p_partner, p_far, p_far_partner, dh, owd = pl.pallas_call(
            chain_kernel,
            out_shape=(shape((tok, dim), F32),) * 4 + (shape((n_loc, rows, 2 * ffn), BF16), shape((n_loc, ffn, dim), F32)),
            in_specs=[vmem_spec] * 8 + [hbm_spec] * 2,
            out_specs=(vmem_spec,) * 5 + (hbm_spec,),
            scratch_shapes=[pltpu.VMEM((4, n_loc, cap, dim), BF16), pltpu.VMEM((2, 2, ffn, dim), F32), pltpu.VMEM((LATE, dim, ffn), BF16), pltpu.VMEM((LATE, dim, ffn), BF16), dma((2,)), dma((2,)), dma((2,))],
            compiler_params=pltpu.CompilerParams(vmem_limit_bytes=18 * MIB),
            cost_estimate=pl.CostEstimate(flops=4_000_000_000, bytes_accessed=20_000_000, transcendentals=0),
            name="chain_kernel",
        )(dd, aa, c1, act, p_all, wg_v, wu_v, wd_v, ins[8], ins[9])

        pairs = [[(i, i ^ k) for i in range(4)] for k in (1, 2, 3)]
        got_fp = lax.ppermute(p_far_partner, "ep", pairs[2])
        got_f = lax.ppermute(p_far, "ep", pairs[1])
        got_p = lax.ppermute(p_partner, "ep", pairs[0])

        owg, owu, ogg = pl.pallas_call(
            weight_kernel,
            out_shape=(shape((n_loc, dim, ffn), F32), shape((n_loc, dim, ffn), F32), shape((top_k, tok), F32)),
            in_specs=[vmem_spec] * 3,
            out_specs=(hbm_spec, hbm_spec, vmem_spec),
            scratch_shapes=[pltpu.VMEM((2, dim, ffn), F32), pltpu.VMEM((2, dim, ffn), F32), dma((2, 2))],
            compiler_params=pltpu.CompilerParams(vmem_limit_bytes=16 * MIB),
            cost_estimate=pl.CostEstimate(flops=16_000_000_000, bytes_accessed=56_000_000, transcendentals=0),
            name="weight_kernel",
        )(x_disp, dh, gg)
        grad_x = (p_own + got_p + got_f + got_fp).astype(BF16)
        return grad_x, ogg.T, owg, owu, owd

    return jax.shard_map(local_step, mesh=mesh, in_specs=(rows_spec, rows_spec, rows_spec, rows_spec, rows_spec, cube_spec, cube_spec, cube_spec, cube_spec, weight_spec, weight_spec, weight_spec), out_specs=(rows_spec, rows_spec, cube_spec, cube_spec, cube_spec), check_vma=False)
```

```python
import jax
import jax.numpy as jnp
from jax import lax
from jax.experimental import pallas as pl
from jax.experimental.pallas import tpu as pltpu
from jax.sharding import PartitionSpec as P

MESH_ID = pl.DeviceIdType.MESH
F32 = jnp.float32
BF16 = jnp.bfloat16
NT = (((1,), (1,)), ((), ()))
TN = (((0,), (0,)), ((), ()))
MIB = 1024 * 1024
COLS = 256
LATE = 2


def peer_ids():
    me = lax.axis_index("ep")
    partner = me + 1 - 2 * lax.rem(me, 2)
    return me, partner, lax.rem(me + 2, 4), lax.rem(partner + 2, 4)


def comm_kernel(gy, gv, tk, sl, pc, yr, hg, hu, wg, wu, wd,
                dd, aa, c1, act_o, p_all, wg_v, wu_v, wd_v, gg,
                gy_all, gv_all, tk_all, sl_all, pc_all, yr_v, hg_v, hu_v,
                own_sem, bulk_sem, gs_sem, gr_sem, ss_sem, sr_sem):
    n_loc = wd.shape[0]
    cap = dd.shape[2]
    tok, dim = gy.shape
    half = tok // 2
    early = wg_v.shape[0]
    me, partner, far, far_partner = peer_ids()
    peers = (partner, far, far_partner)

    own = [pltpu.make_async_copy(gy, gy_all.at[me], own_sem.at[0]),
           pltpu.make_async_copy(gv, gv_all.at[me], own_sem.at[1]),
           pltpu.make_async_copy(tk, tk_all.at[me], own_sem.at[2]),
           pltpu.make_async_copy(sl, sl_all.at[me], own_sem.at[3]),
           pltpu.make_async_copy(pc, pc_all.at[me], own_sem.at[4])]
    for c in own:
        c.start()
    barrier = pltpu.get_barrier_semaphore()
    for d in peers:
        pl.semaphore_signal(barrier, inc=1, device_id={"ep": d}, device_id_type=MESH_ID)
    bulk = [pltpu.make_async_copy(src, dst, bulk_sem.at[i]) for i, (src, dst) in enumerate(((hg, hg_v), (hu, hu_v), (yr, yr_v), (wd.at[pl.ds(0, early)], wd_v), (wg.at[pl.ds(0, early)], wg_v), (wu.at[pl.ds(0, early)], wu_v)))]
    for c in bulk:
        c.start(priority=1)
    for c in own:
        c.wait()
    pl.semaphore_wait(barrier, 3)

    def remote(src, dst, ssem, rsem, dev):
        return pltpu.make_async_remote_copy(src_ref=src, dst_ref=dst, send_sem=ssem, recv_sem=rsem, device_id={"ep": dev}, device_id_type=MESH_ID)

    small = []
    to_far = []
    to_partner = remote(gy_all.at[me], gy_all.at[me], gs_sem.at[0], gr_sem.at[0], partner)
    for h in range(2):
        rows = pl.ds(h * half, half)
        to_far.append(remote(gy_all.at[me, rows], gy_all.at[me, rows], gs_sem.at[1 + h], gr_sem.at[1 + h], far_partner))
    for i, d in enumerate(peers):
        for k, ref in enumerate((gv_all, tk_all, sl_all, pc_all)):
            small.append(remote(ref.at[me], ref.at[me], ss_sem.at[i, k], sr_sem.at[i, k], d))
    for c in to_far + small + [to_partner]:
        c.start()

    def build(s):
        ids = tk_all[s]
        slots = sl_all[s]
        gates = gv_all[s]
        counts = pc_all[s]
        lane = lax.broadcasted_iota(jnp.int32, counts.shape, 1)
        row_c = lax.broadcasted_iota(jnp.int32, (cap, tok), 0).astype(F32)
        hots, cols = [], []
        for e in range(n_loc):
            g = me * n_loc + e
            cnt = jnp.sum(jnp.where(lane == g, counts.astype(F32), 0.0), axis=1, keepdims=True)
            slots_f = slots.astype(F32)
            ok = (ids == g) & (slots >= 0) & (slots_f < cnt)
            slot_row = jnp.max(jnp.where(ok, slots_f, -1.0), axis=0, keepdims=True)
            gate_row = jnp.sum(jnp.where(ok, gates, 0.0), axis=0, keepdims=True)
            hit = row_c == slot_row
            cols.append(jnp.sum(jnp.where(hit, gate_row, 0.0), axis=1, keepdims=True))
            hots.append(jnp.where(hit, 1.0, 0.0).astype(BF16))
        hot = jnp.concatenate(hots, axis=0)
        p_all[s] = hot.astype(F32).T.astype(BF16)
        for n in range(0, dim, COLS):
            picked = jnp.dot(hot, gy_all[s, :, n:n + COLS], preferred_element_type=F32)
            for e in range(n_loc):
                dd[e, s, :, n:n + COLS] = (picked[e * cap:(e + 1) * cap] * cols[e]).astype(BF16)

    build(me)

    bulk[0].wait()
    bulk[1].wait()

    def pre(e, carry):
        h1 = hg_v[e].astype(F32)
        h3 = hu_v[e].astype(F32)
        sig = jax.nn.sigmoid(h1)
        act = h1 * sig
        aa[e] = (act * h3).T.astype(BF16)
        c1[e] = h3 * sig * (1.0 + h1 * (1.0 - sig))
        act_o[e] = act
        return carry

    lax.fori_loop(0, n_loc, pre, 0)

    bulk[2].wait()
    top_k = yr.shape[1]
    dots = lax.dot_general(yr_v[...].reshape(tok * top_k, dim), gy_all[me], NT, preferred_element_type=F32).reshape(tok, top_k, tok)
    same = lax.broadcasted_iota(jnp.int32, dots.shape, 0) == lax.broadcasted_iota(jnp.int32, dots.shape, 2)
    gg[...] = jnp.sum(jnp.where(same, dots, 0.0), axis=0)

    for k in range(4):
        small[k].wait_recv()
    to_partner.wait_recv()
    build(partner)

    relay = []
    for h in range(2):
        rows = pl.ds(h * half, half)
        to_far[h].wait_recv()
        c = remote(gy_all.at[far_partner, rows], gy_all.at[far_partner, rows], gs_sem.at[3 + h], gr_sem.at[3 + h], partner)
        c.start()
        relay.append(c)
    for k in range(4):
        small[8 + k].wait_recv()
    build(far_partner)
    for k in range(4):
        small[4 + k].wait_recv()
    for h in range(2):
        relay[h].wait_recv()
    build(far)

    for c in bulk[3:]:
        c.wait()
    for c in small + to_far + [to_partner] + relay:
        c.wait_send()


def chain_kernel(dd, aa, c1, act, p_all, wg, wu, wd, wg_hbm, wu_hbm, wd_hbm, p_own, p_partner, p_far, p_far_partner, dh, owd, r_all, buf_d, wg_l, wu_l, wd_l, out_sem, in_sem, tail_sem):
    n_loc, _, cap, dim = dd.shape
    ffn = aa.shape[1]
    early = wg.shape[0]
    pairs = n_loc // 2
    ins = [pltpu.make_async_copy(wd_hbm.at[pl.ds(early, LATE)], wd_l, in_sem.at[2]), pltpu.make_async_copy(wg_hbm.at[pl.ds(early, LATE)], wg_l, in_sem.at[0]), pltpu.make_async_copy(wu_hbm.at[pl.ds(early, LATE)], wu_l, in_sem.at[1])]
    for c in ins:
        c.start()

    def down_weight(e, n, k):
        return wd[e, n:n + COLS, k:k + COLS] if e < early else wd_l[e - early, n:n + COLS, k:k + COLS]

    def first(ea, eb, n, side):
        acc = [None] * 2
        for k in range(0, dim, COLS):
            terms = [lax.dot_general(dd[e, :, :, k:k + COLS].reshape(4 * cap, COLS), down_weight(e, n, k), NT, preferred_element_type=F32) for e in (ea, eb)]
            acc = [x if a is None else a + x for a, x in zip(acc, terms)]
            for work in side[k // COLS]:
                work()
        for e, da in zip((ea, eb), acc):
            da = da.astype(BF16).astype(F32)
            dh[e, :, n:n + COLS] = (da * c1[e, :, n:n + COLS]).astype(BF16)
            dh[e, :, ffn + n:ffn + n + COLS] = (da * act[e, :, n:n + COLS]).astype(BF16)

    def gate_up_weight(e, n, k):
        ref = (wg, wu) if e < early else (wg_l, wu_l)
        return ref[k // ffn][e if e < early else e - early, n:n + COLS, k % ffn:k % ffn + COLS]

    def second(ea, eb, na, nb):
        acc = [None] * 4
        for k in range(0, 2 * ffn, COLS):
            terms = [lax.dot_general(dh[ea, :, k:k + COLS], gate_up_weight(ea, n, k), NT, preferred_element_type=F32) for n in (na, nb)]
            terms += [lax.dot_general(gate_up_weight(eb, n, k), dh[eb, :, k:k + COLS], NT, preferred_element_type=F32) for n in (na, nb)]
            acc = [x if a is None else a + x for a, x in zip(acc, terms)]
        for i, n in enumerate((na, nb)):
            ra = acc[i].astype(BF16)
            rb = acc[2 + i].astype(BF16).T
            for s in range(4):
                r_all[s, ea, :, n:n + COLS] = ra[s * cap:(s + 1) * cap]
                r_all[s, eb, :, n:n + COLS] = rb[s * cap:(s + 1) * cap]

    def down(e, n, m):
        def work():
            buf_d[(e // 2) % 2, e % 2, m:m + COLS, n:n + COLS] = jnp.dot(aa[e, m:m + COLS], dd[e, :, :, n:n + COLS].reshape(4 * cap, COLS), preferred_element_type=F32)
        return work

    outs = [pltpu.make_async_copy(buf_d.at[p % 2], owd.at[pl.ds(2 * p, 2)], out_sem.at[p % 2]) for p in range(pairs - 1)]
    tail = [pltpu.make_async_copy(buf_d.at[(pairs - 1) % 2, i], owd.at[n_loc - 2 + i], tail_sem.at[i]) for i in range(2)]
    for p in range(-1, pairs):
        ea, eb = 2 * p, 2 * p + 1
        if 1 <= p < pairs - 1:
            outs[p - 1].wait()
        if p == pairs - 2:
            ins[0].wait()
        if p == pairs - 1:
            for c in ins[1:]:
                c.wait()
        if p >= 0:
            for n in range(0, dim, 2 * COLS):
                second(ea, eb, n, n + COLS)
        if p + 1 < pairs:
            side = [down(ea + 2 + i, n, m) for i in range(2) for n in range(0, dim, COLS) for m in range(0, ffn, COLS)]
            for h, n in enumerate(range(0, ffn, COLS)):
                first(ea + 2, eb + 2, n, [side[8 * h + 2 * q:8 * h + 2 * q + 2] for q in range(4)])
                if p + 2 == pairs:
                    tail[h].start()
            if p + 2 < pairs:
                outs[p + 1].start()

    me, partner, far, far_partner = peer_ids()
    for s, ref in ((me, p_own), (partner, p_partner), (far, p_far), (far_partner, p_far_partner)):
        ref[...] = jnp.dot(p_all[s], r_all[s].reshape(n_loc * cap, dim), preferred_element_type=F32)
    for c in outs[-1:] + tail:
        c.wait()


def weight_kernel(x, dh, gg, owg, owu, ogg, buf, out_sem):
    n_loc, _, dim = x.shape
    ffn = owg.shape[2]
    half = dim // 2
    ogg[...] = gg[...]

    def out_copy(e, slot, k):
        out = (owg, owu)[k % 2]
        rows = pl.ds(k // 2 * half, half)
        return pltpu.make_async_copy(buf.at[slot, k], out.at[e, rows], out_sem.at[slot, k])

    def expert(e, carry):
        slot = lax.rem(e, 2)
        for k in range(4):
            @pl.when(e >= 2)
            def _():
                out_copy(e - 2, slot, k).wait()
            lhs = x[e, :, k // 2 * half:(k // 2 + 1) * half]
            buf[slot, k] = lax.dot_general(lhs, dh[e, :, k % 2 * ffn:(k % 2 + 1) * ffn], TN, preferred_element_type=F32)
            out_copy(e, slot, k).start()
        return carry

    lax.fori_loop(0, n_loc, expert, 0)
    for e in (n_loc - 2, n_loc - 1):
        for k in range(4):
            out_copy(e, e % 2, k).wait()


def solution(mesh):
    rows_spec = P(("dp", "ep"), None)
    cube_spec = P(("dp", "ep"), None, None)
    weight_spec = P("ep", None, None)

    def local_step(grad_y, gate_vals, topk_idx, slot_ids, pair_counts, y_routed, x_disp, h_gate, h_up, w_gate, w_up, w_down):
        tok, dim = grad_y.shape
        top_k = topk_idx.shape[1]
        n_loc, _, ffn = w_gate.shape
        rows = x_disp.shape[1]
        cap = rows // 4
        n_exp = pair_counts.shape[1]
        hbm_spec = pl.BlockSpec(memory_space=pltpu.HBM)
        any_spec = pl.BlockSpec(memory_space=pl.ANY)
        vmem_spec = pl.BlockSpec(memory_space=pltpu.VMEM)
        dma = pltpu.SemaphoreType.DMA
        shape = jax.ShapeDtypeStruct
        ins = [pltpu.with_memory_space_constraint(a, pltpu.HBM) for a in (grad_y, gate_vals.T, topk_idx.T, slot_ids.T, pair_counts, y_routed, h_gate, h_up, w_gate, w_up, w_down)]
        dd, aa, c1, act, p_all, wg_v, wu_v, wd_v, gg = pl.pallas_call(
            comm_kernel,
            out_shape=(shape((n_loc, 4, cap, dim), BF16), shape((n_loc, ffn, rows), BF16), shape((n_loc, rows, ffn), F32), shape((n_loc, rows, ffn), F32),
                       shape((4, tok, n_loc * cap), BF16), shape((n_loc - LATE, dim, ffn), BF16), shape((n_loc - LATE, dim, ffn), BF16), shape((n_loc - LATE, ffn, dim), BF16), shape((top_k, tok), F32)),
            in_specs=[hbm_spec] * 11,
            out_specs=(vmem_spec,) * 9,
            scratch_shapes=[
                pltpu.VMEM((4, tok, dim), BF16), pltpu.VMEM((4, top_k, tok), F32), pltpu.VMEM((4, top_k, tok), jnp.int32), pltpu.VMEM((4, top_k, tok), jnp.int32), pltpu.VMEM((4, 1, n_exp), jnp.int32),
                pltpu.VMEM((tok, top_k, dim), BF16), pltpu.VMEM((n_loc, rows, ffn), BF16), pltpu.VMEM((n_loc, rows, ffn), BF16),
                dma((5,)), dma((6,)), dma((5,)), dma((5,)), dma((3, 4)), dma((3, 4)),
            ],
            compiler_params=pltpu.CompilerParams(collective_id=0, has_side_effects=True, vmem_limit_bytes=8 * MIB),
            cost_estimate=pl.CostEstimate(flops=1_000_000_000, bytes_accessed=30_000_000, transcendentals=0),
            name="comm_kernel",
        )(*ins)

        p_own, p_partner, p_far, p_far_partner, dh, owd = pl.pallas_call(
            chain_kernel,
            out_shape=(shape((tok, dim), F32),) * 4 + (shape((n_loc, rows, 2 * ffn), BF16), shape((n_loc, ffn, dim), F32)),
            in_specs=[vmem_spec] * 8 + [hbm_spec] * 3,
            out_specs=(vmem_spec,) * 5 + (hbm_spec,),
            scratch_shapes=[pltpu.VMEM((4, n_loc, cap, dim), BF16), pltpu.VMEM((2, 2, ffn, dim), F32), pltpu.VMEM((LATE, dim, ffn), BF16), pltpu.VMEM((LATE, dim, ffn), BF16), pltpu.VMEM((LATE, ffn, dim), BF16), dma((2,)), dma((3,)), dma((2,))],
            compiler_params=pltpu.CompilerParams(vmem_limit_bytes=20 * MIB),
            cost_estimate=pl.CostEstimate(flops=4_000_000_000, bytes_accessed=20_000_000, transcendentals=0),
            name="chain_kernel",
        )(dd, aa, c1, act, p_all, wg_v, wu_v, wd_v, ins[8], ins[9], ins[10])

        pairs = [[(i, i ^ k) for i in range(4)] for k in (1, 2, 3)]
        got_fp = lax.ppermute(p_far_partner, "ep", pairs[2])
        got_f = lax.ppermute(p_far, "ep", pairs[1])
        got_p = lax.ppermute(p_partner, "ep", pairs[0])

        owg, owu, ogg = pl.pallas_call(
            weight_kernel,
            out_shape=(shape((n_loc, dim, ffn), F32), shape((n_loc, dim, ffn), F32), shape((top_k, tok), F32)),
            in_specs=[vmem_spec] * 3,
            out_specs=(hbm_spec, hbm_spec, vmem_spec),
            scratch_shapes=[pltpu.VMEM((2, 4, dim // 2, ffn), F32), dma((2, 4))],
            compiler_params=pltpu.CompilerParams(vmem_limit_bytes=16 * MIB),
            cost_estimate=pl.CostEstimate(flops=16_000_000_000, bytes_accessed=56_000_000, transcendentals=0),
            name="weight_kernel",
        )(x_disp, dh, gg)
        grad_x = (p_own + got_p + got_f + got_fp).astype(BF16)
        return grad_x, ogg.T, owg, owu, owd

    return jax.shard_map(local_step, mesh=mesh, in_specs=(rows_spec, rows_spec, rows_spec, rows_spec, rows_spec, cube_spec, cube_spec, cube_spec, cube_spec, weight_spec, weight_spec, weight_spec), out_specs=(rows_spec, rows_spec, cube_spec, cube_spec, cube_spec), check_vma=False)
```

```python
import jax
import jax.numpy as jnp
from jax import lax
from jax.experimental import pallas as pl
from jax.experimental.pallas import tpu as pltpu
from jax.sharding import PartitionSpec as P

MESH_ID = pl.DeviceIdType.MESH
F32 = jnp.float32
BF16 = jnp.bfloat16
NT = (((1,), (1,)), ((), ()))
TN = (((0,), (0,)), ((), ()))
MIB = 1024 * 1024
COLS = 256
LATE = 2


def peer_ids():
    me = lax.axis_index("ep")
    partner = me + 1 - 2 * lax.rem(me, 2)
    return me, partner, lax.rem(me + 2, 4), lax.rem(partner + 2, 4)


def comm_kernel(gy, gv, tk, sl, pc, yr, hg, hu, wg, wu, wd,
                dd, aa, c1, act_o, p_all, wg_v, wu_v, wd_v, gg,
                gy_all, gv_all, tk_all, sl_all, pc_all, yr_v, hg_v, hu_v,
                own_sem, bulk_sem, gs_sem, gr_sem, ss_sem, sr_sem):
    n_loc = wd.shape[0]
    cap = dd.shape[2]
    tok, dim = gy.shape
    half = tok // 2
    early = wg_v.shape[0]
    me, partner, far, far_partner = peer_ids()
    peers = (partner, far, far_partner)

    own = [pltpu.make_async_copy(gy, gy_all.at[me], own_sem.at[0]),
           pltpu.make_async_copy(gv, gv_all.at[me], own_sem.at[1]),
           pltpu.make_async_copy(tk, tk_all.at[me], own_sem.at[2]),
           pltpu.make_async_copy(sl, sl_all.at[me], own_sem.at[3]),
           pltpu.make_async_copy(pc, pc_all.at[me], own_sem.at[4])]
    for c in own:
        c.start()
    barrier = pltpu.get_barrier_semaphore()
    for d in peers:
        pl.semaphore_signal(barrier, inc=1, device_id={"ep": d}, device_id_type=MESH_ID)
    bulk = [pltpu.make_async_copy(src, dst, bulk_sem.at[i]) for i, (src, dst) in enumerate(((hg, hg_v), (hu, hu_v), (yr, yr_v), (wd.at[pl.ds(0, early)], wd_v), (wg.at[pl.ds(0, early)], wg_v), (wu.at[pl.ds(0, early)], wu_v)))]
    for c in bulk:
        c.start(priority=1)
    for c in own:
        c.wait()
    pl.semaphore_wait(barrier, 3)

    def remote(src, dst, ssem, rsem, dev):
        return pltpu.make_async_remote_copy(src_ref=src, dst_ref=dst, send_sem=ssem, recv_sem=rsem, device_id={"ep": dev}, device_id_type=MESH_ID)

    small = []
    to_far = []
    to_partner = remote(gy_all.at[me], gy_all.at[me], gs_sem.at[0], gr_sem.at[0], partner)
    for h in range(2):
        rows = pl.ds(h * half, half)
        to_far.append(remote(gy_all.at[me, rows], gy_all.at[me, rows], gs_sem.at[1 + h], gr_sem.at[1 + h], far_partner))
    for i, d in enumerate(peers):
        for k, ref in enumerate((gv_all, tk_all, sl_all, pc_all)):
            small.append(remote(ref.at[me], ref.at[me], ss_sem.at[i, k], sr_sem.at[i, k], d))
    for c in to_far + small + [to_partner]:
        c.start()

    def build(s):
        ids = tk_all[s]
        slots = sl_all[s]
        gates = gv_all[s]
        counts = pc_all[s]
        lane = lax.broadcasted_iota(jnp.int32, counts.shape, 1)
        row_c = lax.broadcasted_iota(jnp.int32, (cap, tok), 0).astype(F32)
        hots, cols = [], []
        for e in range(n_loc):
            g = me * n_loc + e
            cnt = jnp.sum(jnp.where(lane == g, counts.astype(F32), 0.0), axis=1, keepdims=True)
            slots_f = slots.astype(F32)
            ok = (ids == g) & (slots >= 0) & (slots_f < cnt)
            slot_row = jnp.max(jnp.where(ok, slots_f, -1.0), axis=0, keepdims=True)
            gate_row = jnp.sum(jnp.where(ok, gates, 0.0), axis=0, keepdims=True)
            hit = row_c == slot_row
            cols.append(jnp.sum(jnp.where(hit, gate_row, 0.0), axis=1, keepdims=True))
            hots.append(jnp.where(hit, 1.0, 0.0).astype(BF16))
        hot = jnp.concatenate(hots, axis=0)
        p_all[s] = hot.astype(F32).T.astype(BF16)
        for n in range(0, dim, COLS):
            picked = jnp.dot(hot, gy_all[s, :, n:n + COLS], preferred_element_type=F32)
            for e in range(n_loc):
                dd[e, s, :, n:n + COLS] = (picked[e * cap:(e + 1) * cap] * cols[e]).astype(BF16)

    build(me)

    bulk[0].wait()
    bulk[1].wait()

    def pre(e, carry):
        h1 = hg_v[e].astype(F32)
        h3 = hu_v[e].astype(F32)
        sig = jax.nn.sigmoid(h1)
        act = h1 * sig
        aa[e] = (act * h3).T.astype(BF16)
        c1[e] = h3 * sig * (1.0 + h1 * (1.0 - sig))
        act_o[e] = act
        return carry

    lax.fori_loop(0, n_loc, pre, 0)

    bulk[2].wait()
    top_k = yr.shape[1]
    dots = lax.dot_general(yr_v[...].reshape(tok * top_k, dim), gy_all[me], NT, preferred_element_type=F32).reshape(tok, top_k, tok)
    same = lax.broadcasted_iota(jnp.int32, dots.shape, 0) == lax.broadcasted_iota(jnp.int32, dots.shape, 2)
    gg[...] = jnp.sum(jnp.where(same, dots, 0.0), axis=0)

    for k in range(4):
        small[k].wait_recv()
    to_partner.wait_recv()
    build(partner)

    relay = []
    for h in range(2):
        rows = pl.ds(h * half, half)
        to_far[h].wait_recv()
        c = remote(gy_all.at[far_partner, rows], gy_all.at[far_partner, rows], gs_sem.at[3 + h], gr_sem.at[3 + h], partner)
        c.start()
        relay.append(c)
    for k in range(4):
        small[8 + k].wait_recv()
    build(far_partner)
    for k in range(4):
        small[4 + k].wait_recv()
    for h in range(2):
        relay[h].wait_recv()
    build(far)

    for c in bulk[3:]:
        c.wait()
    for c in small + to_far + [to_partner] + relay:
        c.wait_send()


def chain_kernel(dd, aa, c1, act, p_all, wg, wu, wd, wg_hbm, wu_hbm, wd_hbm, p_own, p_partner, p_far, p_far_partner, dh, owd, r_lo, r_hi, buf_d, wg_l, wu_l, wd_l, out_sem, in_sem, tail_sem):
    n_loc, _, cap, dim = dd.shape
    ffn = aa.shape[1]
    early = wg.shape[0]
    pairs = n_loc // 2
    ins = [pltpu.make_async_copy(wd_hbm.at[pl.ds(early, LATE)], wd_l, in_sem.at[2]), pltpu.make_async_copy(wg_hbm.at[pl.ds(early, LATE)], wg_l, in_sem.at[0]), pltpu.make_async_copy(wu_hbm.at[pl.ds(early, LATE)], wu_l, in_sem.at[1])]
    for c in ins:
        c.start()

    def down_weight(e, n, k):
        return wd[e, n:n + COLS, k:k + COLS] if e < early else wd_l[e - early, n:n + COLS, k:k + COLS]

    def first(ea, eb, n, side):
        acc = [None] * 2
        for k in range(0, dim, COLS):
            terms = [lax.dot_general(dd[e, :, :, k:k + COLS].reshape(4 * cap, COLS), down_weight(e, n, k), NT, preferred_element_type=F32) for e in (ea, eb)]
            acc = [x if a is None else a + x for a, x in zip(acc, terms)]
            for work in side[k // COLS]:
                work()
        for e, da in zip((ea, eb), acc):
            da = da.astype(BF16).astype(F32)
            dh[e, :, n:n + COLS] = (da * c1[e, :, n:n + COLS]).astype(BF16)
            dh[e, :, ffn + n:ffn + n + COLS] = (da * act[e, :, n:n + COLS]).astype(BF16)

    def gate_up_weight(e, n, k):
        ref = (wg, wu) if e < early else (wg_l, wu_l)
        return ref[k // ffn][e if e < early else e - early, n:n + COLS, k % ffn:k % ffn + COLS]

    def second(ea, eb, na, nb):
        acc = [None] * 4
        for k in range(0, 2 * ffn, COLS):
            terms = [lax.dot_general(dh[ea, :, k:k + COLS], gate_up_weight(ea, n, k), NT, preferred_element_type=F32) for n in (na, nb)]
            terms += [lax.dot_general(gate_up_weight(eb, n, k), dh[eb, :, k:k + COLS], NT, preferred_element_type=F32) for n in (na, nb)]
            acc = [x if a is None else a + x for a, x in zip(acc, terms)]
        for i, n in enumerate((na, nb)):
            ra = acc[i].astype(BF16)
            rb = acc[2 + i].astype(BF16).T
            for s in range(4):
                r_half = r_lo if n < dim // 2 else r_hi
                at = n % (dim // 2)
                r_half[s, ea, :, at:at + COLS] = ra[s * cap:(s + 1) * cap]
                r_half[s, eb, :, at:at + COLS] = rb[s * cap:(s + 1) * cap]

    def down(e, n, m):
        def work():
            buf_d[(e // 2) % 2, e % 2, m:m + COLS, n:n + COLS] = jnp.dot(aa[e, m:m + COLS], dd[e, :, :, n:n + COLS].reshape(4 * cap, COLS), preferred_element_type=F32)
        return work

    outs = [pltpu.make_async_copy(buf_d.at[p % 2], owd.at[pl.ds(2 * p, 2)], out_sem.at[p % 2]) for p in range(pairs - 1)]
    tail = [pltpu.make_async_copy(buf_d.at[(pairs - 1) % 2, i], owd.at[n_loc - 2 + i], tail_sem.at[i]) for i in range(2)]
    for p in range(-1, pairs):
        ea, eb = 2 * p, 2 * p + 1
        if 1 <= p < pairs - 1:
            outs[p - 1].wait()
        if p == pairs - 2:
            ins[0].wait()
        if p == pairs - 1:
            for c in ins[1:]:
                c.wait()
        side = [down(ea + 2 + i, n, m) for i in range(2) for n in range(0, dim, COLS) for m in range(0, ffn, COLS)] if p + 1 < pairs else []
        for h in range(2):
            if p >= 0:
                second(ea, eb, 2 * h * COLS, (2 * h + 1) * COLS)
            if p + 1 < pairs:
                first(ea + 2, eb + 2, h * COLS, [side[8 * h + 2 * q:8 * h + 2 * q + 2] for q in range(4)])
                if p + 2 == pairs:
                    tail[h].start()
        if p + 2 < pairs:
            outs[p + 1].start()

    me, partner, far, far_partner = peer_ids()
    for k, r_half in enumerate((r_lo, r_hi)):
        for s, ref in ((me, p_own), (partner, p_partner), (far, p_far), (far_partner, p_far_partner)):
            ref[:, k * dim // 2:(k + 1) * dim // 2] = jnp.dot(p_all[s], r_half[s].reshape(n_loc * cap, dim // 2), preferred_element_type=F32)
    for c in outs[-1:] + tail:
        c.wait()


def weight_kernel(x, dh, gg, owg, owu, ogg, buf, out_sem):
    n_loc, _, dim = x.shape
    ffn = owg.shape[2]
    half = dim // 2
    ogg[...] = gg[...]

    def out_copy(e, slot, k):
        out = (owg, owu)[k % 2]
        rows = pl.ds(k // 2 * half, half)
        return pltpu.make_async_copy(buf.at[slot, k], out.at[e, rows], out_sem.at[slot, k])

    def expert(e, carry):
        slot = lax.rem(e, 2)
        for k in range(4):
            @pl.when(e >= 2)
            def _():
                out_copy(e - 2, slot, k).wait()
            lhs = x[e, :, k // 2 * half:(k // 2 + 1) * half]
            buf[slot, k] = lax.dot_general(lhs, dh[e, :, k % 2 * ffn:(k % 2 + 1) * ffn], TN, preferred_element_type=F32)
            out_copy(e, slot, k).start()
        return carry

    lax.fori_loop(0, n_loc, expert, 0)
    for e in (n_loc - 2, n_loc - 1):
        for k in range(4):
            out_copy(e, e % 2, k).wait()


def solution(mesh):
    rows_spec = P(("dp", "ep"), None)
    cube_spec = P(("dp", "ep"), None, None)
    weight_spec = P("ep", None, None)

    def local_step(grad_y, gate_vals, topk_idx, slot_ids, pair_counts, y_routed, x_disp, h_gate, h_up, w_gate, w_up, w_down):
        tok, dim = grad_y.shape
        top_k = topk_idx.shape[1]
        n_loc, _, ffn = w_gate.shape
        rows = x_disp.shape[1]
        cap = rows // 4
        n_exp = pair_counts.shape[1]
        hbm_spec = pl.BlockSpec(memory_space=pltpu.HBM)
        any_spec = pl.BlockSpec(memory_space=pl.ANY)
        vmem_spec = pl.BlockSpec(memory_space=pltpu.VMEM)
        dma = pltpu.SemaphoreType.DMA
        shape = jax.ShapeDtypeStruct
        ins = [pltpu.with_memory_space_constraint(a, pltpu.HBM) for a in (grad_y, gate_vals.T, topk_idx.T, slot_ids.T, pair_counts, y_routed, h_gate, h_up, w_gate, w_up, w_down)]
        dd, aa, c1, act, p_all, wg_v, wu_v, wd_v, gg = pl.pallas_call(
            comm_kernel,
            out_shape=(shape((n_loc, 4, cap, dim), BF16), shape((n_loc, ffn, rows), BF16), shape((n_loc, rows, ffn), F32), shape((n_loc, rows, ffn), F32),
                       shape((4, tok, n_loc * cap), BF16), shape((n_loc - LATE, dim, ffn), BF16), shape((n_loc - LATE, dim, ffn), BF16), shape((n_loc - LATE, ffn, dim), BF16), shape((top_k, tok), F32)),
            in_specs=[hbm_spec] * 11,
            out_specs=(vmem_spec,) * 9,
            scratch_shapes=[
                pltpu.VMEM((4, tok, dim), BF16), pltpu.VMEM((4, top_k, tok), F32), pltpu.VMEM((4, top_k, tok), jnp.int32), pltpu.VMEM((4, top_k, tok), jnp.int32), pltpu.VMEM((4, 1, n_exp), jnp.int32),
                pltpu.VMEM((tok, top_k, dim), BF16), pltpu.VMEM((n_loc, rows, ffn), BF16), pltpu.VMEM((n_loc, rows, ffn), BF16),
                dma((5,)), dma((6,)), dma((5,)), dma((5,)), dma((3, 4)), dma((3, 4)),
            ],
            compiler_params=pltpu.CompilerParams(collective_id=0, has_side_effects=True, vmem_limit_bytes=8 * MIB),
            cost_estimate=pl.CostEstimate(flops=1_000_000_000, bytes_accessed=30_000_000, transcendentals=0),
            name="comm_kernel",
        )(*ins)

        p_own, p_partner, p_far, p_far_partner, dh, owd = pl.pallas_call(
            chain_kernel,
            out_shape=(shape((tok, dim), F32),) * 4 + (shape((n_loc, rows, 2 * ffn), BF16), shape((n_loc, ffn, dim), F32)),
            in_specs=[vmem_spec] * 8 + [hbm_spec] * 3,
            out_specs=(vmem_spec,) * 5 + (hbm_spec,),
            scratch_shapes=[pltpu.VMEM((4, n_loc, cap, dim // 2), BF16), pltpu.VMEM((4, n_loc, cap, dim // 2), BF16), pltpu.VMEM((2, 2, ffn, dim), F32), pltpu.VMEM((LATE, dim, ffn), BF16), pltpu.VMEM((LATE, dim, ffn), BF16), pltpu.VMEM((LATE, ffn, dim), BF16), dma((2,)), dma((3,)), dma((2,))],
            compiler_params=pltpu.CompilerParams(vmem_limit_bytes=20 * MIB),
            cost_estimate=pl.CostEstimate(flops=4_000_000_000, bytes_accessed=20_000_000, transcendentals=0),
            name="chain_kernel",
        )(dd, aa, c1, act, p_all, wg_v, wu_v, wd_v, ins[8], ins[9], ins[10])

        pairs = [[(i, i ^ k) for i in range(4)] for k in (1, 2, 3)]
        got_fp = lax.ppermute(p_far_partner, "ep", pairs[2])
        got_f = lax.ppermute(p_far, "ep", pairs[1])
        got_p = lax.ppermute(p_partner, "ep", pairs[0])

        owg, owu, ogg = pl.pallas_call(
            weight_kernel,
            out_shape=(shape((n_loc, dim, ffn), F32), shape((n_loc, dim, ffn), F32), shape((top_k, tok), F32)),
            in_specs=[vmem_spec] * 3,
            out_specs=(hbm_spec, hbm_spec, vmem_spec),
            scratch_shapes=[pltpu.VMEM((2, 4, dim // 2, ffn), F32), dma((2, 4))],
            compiler_params=pltpu.CompilerParams(vmem_limit_bytes=16 * MIB),
            cost_estimate=pl.CostEstimate(flops=16_000_000_000, bytes_accessed=56_000_000, transcendentals=0),
            name="weight_kernel",
        )(x_disp, dh, gg)
        grad_x = (p_own + got_p + got_f + got_fp).astype(BF16)
        return grad_x, ogg.T, owg, owu, owd

    return jax.shard_map(local_step, mesh=mesh, in_specs=(rows_spec, rows_spec, rows_spec, rows_spec, rows_spec, cube_spec, cube_spec, cube_spec, cube_spec, weight_spec, weight_spec, weight_spec), out_specs=(rows_spec, rows_spec, cube_spec, cube_spec, cube_spec), check_vma=False)
```
